32 devices in a mesh: seq: 16 (over z, y, core), fsdp: 2 (over x).
Axes of the slice: x: 2, y: 2, z: 4, core: 2. Of those that a mesh axis runs over, the one named last changes fastest.
Arguments:
- tokens: bfloat16 [8192, 5376], P(('seq', 'fsdp')), may hold values from -6 to 6
- norm_gain: float32 [5376], replicated, may hold values from 0.1 to 1.9
- query_weight: bfloat16 [5376, 2048], P('seq', 'fsdp'), may hold values from -0.078125 to 0.078125
- key_matrix: bfloat16 [5376, 1024], P('seq', 'fsdp'), may hold values from -0.078125 to 0.078125
- value_matrix: bfloat16 [5376, 1024], P('seq', 'fsdp'), may hold values from -0.078125 to 0.078125
- out_weight: bfloat16 [5376, 2048], P('seq', 'fsdp'), may hold values from -0.125 to 0.125
- query_gain: float32 [128], replicated, may hold values from 0.1 to 1.9
- key_gain: float32 [128], replicated, may hold values from 0.1 to 1.9
- post_gain: float32 [5376], replicated, may hold values from 0.1 to 1.9
Outputs:
- layer_out: bfloat16 [8192, 5376], P(('seq', 'fsdp'))
The draws below stay inside these ranges and needn't reach their ends.
All inputs are finite; a program needn't handle non-finite values.
Results may differ from the reference program's by a relative error of at most 0.011.
Values may be sent and summed in bfloat16 or wider, within the bound.
A program may use at most 192 MiB of HBM per device.

```python
import jax
import jax.numpy as jnp
from jax import lax

MODEL_WIDTH = 5376
HEAD_SIZE = 128
QUERY_HEADS = 16
KEY_VALUE_HEADS = 8
WINDOW_LENGTH = 1024
TOKENS = 8192
N_FSDP = 2


def levels(rng, extent, split, least, high):
    level = 1.0
    for dim, shards_of in split:
        steps = jax.random.uniform(jax.random.fold_in(jax.random.fold_in(rng, 6), dim), (shards_of,), jnp.float32, least / len(split), high / len(split))
        level = level * jnp.repeat(jnp.exp(steps), extent[dim] // shards_of).reshape((-1,) + (1,) * (len(extent) - 1 - dim))
    return level


def bell_draw(stream_key, dims, scale, most, pieces=(), kind=jnp.bfloat16):
    loudness = levels(stream_key, dims, pieces, -0.22, 0.18) if pieces else 1.0
    drawn = jax.random.normal(stream_key, dims, jnp.float32) * scale * loudness
    return jnp.minimum(jnp.maximum(drawn, -most), most).astype(kind)


def setup_inputs(seed: int = 0) -> dict:
    key_of = jax.random.split(jax.random.key(seed), 10)
    return {
        "tokens": bell_draw(key_of[0], (TOKENS, MODEL_WIDTH), 1.0, 6.0, ((0, 32),)),
        "norm_gain": jnp.clip(1.0 + 0.18 * jax.random.normal(key_of[1], (MODEL_WIDTH,), jnp.float32), 0.1, 1.9),
        "query_weight": bell_draw(key_of[2], (MODEL_WIDTH, QUERY_HEADS * HEAD_SIZE), MODEL_WIDTH ** -0.5, 0.078125, ((0, 16), (1, 2))),
        "key_matrix": bell_draw(key_of[3], (MODEL_WIDTH, KEY_VALUE_HEADS * HEAD_SIZE), MODEL_WIDTH ** -0.5, 0.078125, ((0, 16), (1, 2))),
        "value_matrix": bell_draw(key_of[4], (MODEL_WIDTH, KEY_VALUE_HEADS * HEAD_SIZE), MODEL_WIDTH ** -0.5, 0.078125, ((0, 16), (1, 2))),
        "out_weight": bell_draw(key_of[5], (MODEL_WIDTH, QUERY_HEADS * HEAD_SIZE), (QUERY_HEADS * HEAD_SIZE) ** -0.5, 0.125, ((0, 16), (1, 2))),
        "query_gain": jnp.clip(1.0 + 0.18 * jax.random.normal(key_of[6], (HEAD_SIZE,), jnp.float32), 0.1, 1.9),
        "key_gain": jnp.clip(1.0 + 0.18 * jax.random.normal(key_of[7], (HEAD_SIZE,), jnp.float32), 0.1, 1.9),
        "post_gain": jnp.clip(1.0 + 0.18 * jax.random.normal(key_of[8], (MODEL_WIDTH,), jnp.float32), 0.1, 1.9),
    }


epsilon = 1e-06
score_scale = 168.0 ** (-0.5)
rope_base = 10000.0
masked_score = -1e+30

def rms_scaled(values, gain):
    mean_square = lax.optimization_barrier(jnp.mean(values * values, axis=-1, keepdims=True))
    return values * lax.rsqrt(mean_square + epsilon) * gain

def rotary(values, positions):
    half_width = values.shape[-1] // 2
    exponents = jnp.arange(half_width, dtype=jnp.float32) * (2.0 / values.shape[-1])
    frequency = jnp.exp(-exponents * jnp.log(jnp.float32(rope_base)))
    angles = positions.astype(jnp.float32)[:, None] * frequency[None, :]
    cosine = jnp.cos(angles)[:, None, :]
    sine = jnp.sin(angles)[:, None, :]
    first_half = values[..., :half_width]
    second_half = values[..., half_width:]
    return jnp.concatenate([first_half * cosine - second_half * sine, second_half * cosine + first_half * sine], axis=-1)

def head_states(projected, gain, positions):
    shaped = projected.reshape(projected.shape[0], -1, HEAD_SIZE)
    return rotary(rms_scaled(shaped, gain), positions).astype(jnp.bfloat16)

def window_block(query_block, key_block, value_block, query_pos, key_pos):
    scores = jnp.einsum('rkgd,lkd->kgrl', query_block.astype(jnp.float32), key_block.astype(jnp.float32), precision=lax.Precision.HIGHEST) * score_scale
    offset = query_pos[:, None] - key_pos[None, :]
    allowed = (offset >= 0) & (offset < WINDOW_LENGTH) & (key_pos[None, :] >= 0)
    scores = jnp.where(allowed, scores, masked_score)
    highest = lax.optimization_barrier(jnp.max(scores, axis=-1, keepdims=True))
    raised = jnp.exp(scores - highest)
    weights = (raised / lax.optimization_barrier(jnp.sum(raised, axis=-1, keepdims=True))).astype(jnp.bfloat16)
    mixed = jnp.einsum('kgrl,lkd->rkgd', weights.astype(jnp.float32), value_block.astype(jnp.float32), precision=lax.Precision.HIGHEST)
    return mixed.astype(jnp.bfloat16).reshape(query_block.shape[0], -1)

def reference(tokens, norm_gain, query_weight, key_matrix, value_matrix, out_weight, query_gain, key_gain, post_gain):
    row_count = tokens.shape[0]
    query_groups = QUERY_HEADS // KEY_VALUE_HEADS
    normed_input = rms_scaled(tokens.astype(jnp.float32), norm_gain).astype(jnp.bfloat16)
    positions = jnp.arange(row_count, dtype=jnp.int32)
    query_states = head_states(jnp.dot(normed_input, query_weight, preferred_element_type=jnp.float32), query_gain, positions)
    query_states = query_states.reshape(row_count, KEY_VALUE_HEADS, query_groups, HEAD_SIZE)
    keys_all = head_states(jnp.dot(normed_input, key_matrix, preferred_element_type=jnp.float32), key_gain, positions)
    value_states = jnp.dot(normed_input, value_matrix, preferred_element_type=jnp.float32).astype(jnp.bfloat16).reshape(row_count, KEY_VALUE_HEADS, HEAD_SIZE)
    padding_rows = jnp.zeros((WINDOW_LENGTH, KEY_VALUE_HEADS, HEAD_SIZE), jnp.bfloat16)
    padded_keys = jnp.concatenate([padding_rows, keys_all], axis=0)
    padded_values = jnp.concatenate([padding_rows, value_states], axis=0)

    def one_block(block_index):
        begin = (block_index * WINDOW_LENGTH).astype(jnp.int32)
        query_block = lax.dynamic_slice_in_dim(query_states, begin, WINDOW_LENGTH, 0)
        key_block = lax.dynamic_slice_in_dim(padded_keys, begin, 2 * WINDOW_LENGTH, 0)
        value_block = lax.dynamic_slice_in_dim(padded_values, begin, 2 * WINDOW_LENGTH, 0)
        query_pos = begin + jnp.arange(WINDOW_LENGTH, dtype=jnp.int32)
        key_pos = begin - WINDOW_LENGTH + jnp.arange(2 * WINDOW_LENGTH, dtype=jnp.int32)
        return window_block(query_block, key_block, value_block, query_pos, key_pos)
    blocks = lax.map(one_block, jnp.arange(row_count // WINDOW_LENGTH, dtype=jnp.int32))
    attended = blocks.reshape(row_count, QUERY_HEADS * HEAD_SIZE)
    group_width = QUERY_HEADS * HEAD_SIZE // N_FSDP
    projected = jnp.zeros((row_count, out_weight.shape[0]), jnp.float32)
    for group in range(N_FSDP):
        left = attended[:, group * group_width:(group + 1) * group_width]
        right = out_weight[:, group * group_width:(group + 1) * group_width]
        term = lax.dot_general(left, right, (((1,), (1,)), ((), ())), preferred_element_type=jnp.float32)
        projected = projected + term.astype(jnp.bfloat16).astype(jnp.float32)
    return (tokens.astype(jnp.float32) + rms_scaled(projected, post_gain)).astype(jnp.bfloat16)
```

```python
import functools

import jax
import jax.numpy as jnp
from jax import lax
from jax.experimental import pallas as pl
from jax.experimental.pallas import tpu as pltpu
from jax.sharding import PartitionSpec as P

HEAD_SIZE = 128
WINDOW_LENGTH = 1024

epsilon = 1e-06
score_scale = 168.0 ** (-0.5)
log2_e = 1.4426950408889634
rope_base = 10000.0
pieces = 2
token_pieces = 4
MESH = pl.DeviceIdType.MESH


def ring_place(chip, chips):
    row, side = chip // 2, chip % 2
    return side * (chips - 1 - row) + (1 - side) * row


def ring_chip(place, chips):
    back = place // (chips // 2)
    return back * (2 * (chips - 1 - place) + 1) + (1 - back) * 2 * place


class Ring:
    def __init__(self, shards, sems):
        self.chips = shards // 2
        self.me = lax.axis_index("seq")
        self.group = lax.axis_index("fsdp")
        self.core = self.me % 2
        self.place = ring_place(self.me // 2, self.chips)
        self.other = (self.me // 2) * 2 + 1 - self.core
        self.ahead = self.neighbour(1)
        self.behind = self.neighbour(self.chips - 1)
        self.ring_send, self.ring_recv, self.pair_send, self.pair_recv = sems

    def neighbour(self, distance):
        return ring_chip((self.place + distance) % self.chips, self.chips) * 2 + self.core

    def owner(self, way, step):
        return ring_chip((self.place + (self.chips - way) * step) % self.chips, self.chips)

    def ring_copy(self, flow, step):
        index, slot_of, way = flow
        slot = slot_of(self.owner(way, step), self.core)
        return pltpu.make_async_remote_copy(
            src_ref=slot,
            dst_ref=slot,
            send_sem=self.ring_send.at[index, step],
            recv_sem=self.ring_recv.at[index, step],
            device_id=(self.ahead if way > 0 else self.behind, self.group),
            device_id_type=MESH,
        )

    def arrival(self, flow, step):
        index, slot_of, way = flow
        slot = slot_of(self.owner(way, step), self.core)
        return pltpu.make_async_remote_copy(
            src_ref=slot,
            dst_ref=slot,
            send_sem=self.ring_send.at[index, step - 1],
            recv_sem=self.ring_recv.at[index, step - 1],
            device_id=(self.ahead if way > 0 else self.behind, self.group),
            device_id_type=MESH,
        )

    def pair_copy(self, flow, step, core):
        index, slot_of, way = flow
        slot = slot_of(self.owner(way, step), core)
        return pltpu.make_async_remote_copy(
            src_ref=slot,
            dst_ref=slot,
            send_sem=self.pair_send.at[index, step],
            recv_sem=self.pair_recv.at[index, step],
            device_id=(self.other, self.group),
            device_id_type=MESH,
        )

    def hop(self, flows, step, first=False, last=False):
        for flow in flows:
            if not first:
                self.arrival(flow, step).wait_recv()
            if not last:
                self.ring_copy(flow, step).start()
            self.pair_copy(flow, step, self.core).start()

    def landed(self, flows, step):
        for flow in flows:
            self.pair_copy(flow, step, 1 - self.core).wait_recv()

    def drain(self, flows):
        def one(step, carry):
            for flow in flows:
                self.ring_copy(flow, step).wait_send()
                self.pair_copy(flow, step, self.core).wait_send()
            return carry

        lax.fori_loop(0, self.chips - 1, one, 0)
        for flow in flows:
            self.pair_copy(flow, self.chips - 1, self.core).wait_send()


def turned(values, gain, cosine, sine, scale):
    mean_square = jnp.mean(values * values, axis=-1, keepdims=True)
    normed = values * lax.rsqrt(mean_square + epsilon) * gain
    swapped = pltpu.roll(normed, values.shape[-1] // 2, 1)
    return (normed * cosine + swapped * sine) * scale


def project_kernel(
    shards,
    merge,
    tokens_ref,
    gain_ref,
    query_ref,
    key_ref,
    value_ref,
    out_ref,
    query_gain_ref,
    key_gain_ref,
    cosine_ref,
    sine_ref,
    query_out,
    key_out,
    value_out,
    swap_out,
    query_land,
    key_land,
    value_land,
    raw,
    split,
    query_sum,
    key_sum,
    value_sum,
    key_own,
    value_own,
    ring_send,
    ring_recv,
    pair_send,
    pair_recv,
    local_sem,
    token_send,
    token_recv,
    swap_sem,
    far_send,
    far_recv,
    near_send,
    near_recv,
):
    ring = Ring(shards, (ring_send, ring_recv, pair_send, pair_recv))
    chips, me, group, core = ring.chips, ring.me, ring.group, ring.core
    rows = key_ref.shape[0]
    part_rows = tokens_ref.shape[0]
    width = key_ref.shape[1]
    half = query_ref.shape[1] // 2
    far_to = (me + 2) % shards
    far_from = (me + shards - 2) % shards

    barrier = pltpu.get_barrier_semaphore()
    for device in (ring.other, ring.ahead, ring.behind, far_to, far_from):
        pl.semaphore_signal(barrier, inc=1, device_id=(device, group), device_id_type=MESH)
    pl.semaphore_signal(barrier, inc=1, device_id=(me, 1 - group), device_id_type=MESH)

    @pl.when(core != group)
    def _():
        pl.semaphore_signal(
            barrier,
            inc=1,
            device_id=((me // 2) * 2 + group, core),
            device_id_type=MESH,
        )

    local = [
        pltpu.make_async_copy(key_ref, key_land.at[me], local_sem.at[0]),
        pltpu.make_async_copy(value_ref, value_land.at[me], local_sem.at[1]),
        pltpu.make_async_copy(query_ref, query_land.at[me], local_sem.at[2]),
        pltpu.make_async_copy(tokens_ref, raw.at[group], local_sem.at[3]),
    ]
    for copy in local:
        copy.start()
    pl.semaphore_wait(barrier, 6 + (core + group) % 2)

    def flow(index, land, column, count, way):
        return index, lambda chip, side: land.at[chip * 2 + side, :, pl.ds(column, count)], way

    size, wide = width // pieces, half // pieces
    first_flows, second_flows = [], []
    for piece in range(pieces):
        first_flows.append(flow(2 * piece, key_land, piece * size, size, 1))
        first_flows.append(flow(2 * piece + 1, value_land, piece * size, size, -1))
    for piece in range(pieces):
        base = 2 * (pieces + piece)
        second_flows.append(flow(base, query_land, piece * wide, wide, 1))
        second_flows.append(flow(base + 1, query_land, half + piece * wide, wide, -1))

    token_rows = part_rows // token_pieces

    def token_copy(piece, side):
        span = pl.ds(piece * token_rows, token_rows)
        return pltpu.make_async_remote_copy(
            src_ref=tokens_ref.at[span],
            dst_ref=raw.at[side, span],
            send_sem=token_send.at[piece],
            recv_sem=token_recv.at[piece],
            device_id=(me, 1 - group),
            device_id_type=MESH,
        )

    swap = pltpu.make_async_remote_copy(
        src_ref=out_ref,
        dst_ref=swap_out,
        send_sem=swap_sem.at[0],
        recv_sem=swap_sem.at[1],
        device_id=((me // 2) * 2 + group, core),
        device_id_type=MESH,
    )

    local[0].wait()
    local[1].wait()
    ring.hop(first_flows, 0, first=True)
    for piece in range(token_pieces):
        token_copy(piece, group).start()

    @pl.when(core != group)
    def _():
        swap.start()

    local[2].wait()
    local[3].wait()

    block = 16
    span_width = rows * merge

    def normed_rows(side, begin, count):
        def one(index, carry):
            start = pl.multiple_of(begin + index * block, block)
            values = raw[side, pl.ds(start, block), :].astype(jnp.float32)
            mean_square = jnp.mean(values * values, axis=-1, keepdims=True)
            normed = values * lax.rsqrt(mean_square + epsilon) * gain_ref[...]
            target = pl.multiple_of(side * part_rows + start, block)
            for part in range(shards // merge):
                piece = normed[:, part * span_width : (part + 1) * span_width]
                split[part, pl.ds(target, block), :] = piece.astype(jnp.bfloat16)
            return carry

        lax.fori_loop(0, count // block, one, 0)

    normed_rows(group, 0, part_rows)
    key_sum[...] = jnp.zeros_like(key_sum)
    value_sum[...] = jnp.zeros_like(value_sum)
    query_sum[...] = jnp.zeros_like(query_sum)

    def products(total, columns, land, chip):
        if merge == 2:
            weights = land[pl.ds(chip * 2, 2), :, columns]
            weights = weights.reshape(2 * rows, weights.shape[-1])
            total[:, columns] += jnp.dot(
                split[chip], weights, preferred_element_type=jnp.float32
            )
        else:
            for side in range(2):
                total[:, columns] += jnp.dot(
                    split[chip * 2 + side],
                    land[chip * 2 + side, :, columns],
                    preferred_element_type=jnp.float32,
                )

    def key_value(step, carry):
        everything = pl.ds(0, width)
        products(key_sum, everything, key_land, ring.owner(1, step))
        products(value_sum, everything, value_land, ring.owner(-1, step))
        return carry

    def query(step, carry):
        products(query_sum, pl.ds(0, half), query_land, ring.owner(1, step))
        products(query_sum, pl.ds(half, half), query_land, ring.owner(-1, step))
        return carry

    def first_step(step, carry):
        ring.hop(first_flows, step)
        return carry

    lax.fori_loop(1, chips - 1, first_step, 0)
    ring.hop(second_flows, 0, first=True)
    ring.hop(first_flows, chips - 1, last=True)
    for piece in range(token_pieces - 1):
        token_copy(piece, 1 - group).wait_recv()
    normed_rows(1 - group, 0, part_rows - token_rows)

    def settle(step, carry):
        ring.landed(first_flows, step)
        return carry

    lax.fori_loop(0, chips, settle, 0)

    heads = width // HEAD_SIZE
    query_heads = query_ref.shape[1] // HEAD_SIZE

    def far_copy(index, own, target):
        return pltpu.make_async_remote_copy(
            src_ref=own,
            dst_ref=target.at[0],
            send_sem=far_send.at[index],
            recv_sem=far_recv.at[index],
            device_id=(far_to, group),
            device_id_type=MESH,
        )

    def near_copy(index, source, target):
        return pltpu.make_async_remote_copy(
            src_ref=source,
            dst_ref=target.at[1],
            send_sem=near_send.at[index],
            recv_sem=near_recv.at[index],
            device_id=(ring.other, group),
            device_id_type=MESH,
        )

    stacks = ((0, key_own, key_out), (1, value_own, value_out))

    def keep(index, own, target):
        return pltpu.make_async_copy(own, target.at[2], local_sem.at[index])

    def finish_keys():
        def one(head, carry):
            columns = pl.ds(pl.multiple_of(head * HEAD_SIZE, HEAD_SIZE), HEAD_SIZE)
            key_own[:, columns] = turned(
                key_sum[:, columns], key_gain_ref[...], cosine_ref[...], sine_ref[...], 1.0
            ).astype(jnp.bfloat16)
            return carry

        value_own[...] = value_sum[...].astype(jnp.bfloat16)
        lax.fori_loop(0, heads, one, 0)

    def send_keys():
        for index, own, target in stacks:
            keep(index, own, target).start()

            @pl.when(me + 2 < shards)
            def _():
                far_copy(index, own, target).start()

            @pl.when(core == 0)
            def _():
                near_copy(index, own, target).start()

    def second_step(step, carry):
        ring.hop(second_flows, step)
        ring.landed(second_flows, step - 1)

        @pl.when(step == 1)
        def _():
            token_copy(token_pieces - 1, 1 - group).wait_recv()
            normed_rows(1 - group, part_rows - token_rows, token_rows)
            lax.fori_loop(0, chips // 2, key_value, 0)

        @pl.when(step == 2)
        def _():
            lax.fori_loop(chips // 2, chips, key_value, 0)
            finish_keys()

        @pl.when(step == 3)
        def _():
            query(0, 0)
            send_keys()
            lax.fori_loop(1, 3, query, 0)

        @pl.when(step > 3)
        def _():
            query(step - 1, 0)

        return carry

    lax.fori_loop(1, chips - 1, second_step, 0)
    ring.hop(second_flows, chips - 1, last=True)
    ring.landed(second_flows, chips - 2)
    query(chips - 2, 0)

    @pl.when(me >= 2)
    def _():
        for index, own, target in stacks:
            far_copy(index, own, target).wait_recv()

            @pl.when(core == 1)
            def _():
                near_copy(index, target.at[0], target).start()

    ring.landed(second_flows, chips - 1)
    query(chips - 1, 0)

    def finish_query(head, carry):
        columns = pl.ds(pl.multiple_of(head * HEAD_SIZE, HEAD_SIZE), HEAD_SIZE)
        query_out[:, columns] = turned(
            query_sum[:, columns],
            query_gain_ref[...],
            cosine_ref[...],
            sine_ref[...],
            score_scale * log2_e,
        ).astype(jnp.bfloat16)
        return carry

    lax.fori_loop(0, query_heads, finish_query, 0)

    for index, own, target in stacks:
        keep(index, own, target).wait()

        @pl.when(me + 2 < shards)
        def _():
            far_copy(index, own, target).wait_send()

        @pl.when(core == 0)
        def _():
            near_copy(index, own, target).wait_send()

            @pl.when(me >= 2)
            def _():
                near_copy(index, own, target).wait_recv()

        @pl.when(core == 1)
        def _():
            near_copy(index, own, target).wait_recv()

            @pl.when(me >= 2)
            def _():
                near_copy(index, target.at[0], target).wait_send()

    for piece in range(token_pieces):
        token_copy(piece, group).wait_send()

    @pl.when(core != group)
    def _():
        swap.wait()

    ring.drain(first_flows)
    ring.drain(second_flows)


def attend_kernel(
    shards,
    query_ref,
    key_ref,
    value_ref,
    out_ref,
    swap_ref,
    tokens_ref,
    gain_ref,
    result_ref,
    out_land,
    key_window,
    value_window,
    attended,
    projected,
    gathered,
    ring_send,
    ring_recv,
    pair_send,
    pair_recv,
    load_sem,
    mixed_send,
    mixed_recv,
    back_send,
    back_recv,
):
    ring = Ring(shards, (ring_send, ring_recv, pair_send, pair_recv))
    chips, me, group, core = ring.chips, ring.me, ring.group, ring.core
    shard_rows = key_ref.shape[1]
    part_rows = tokens_ref.shape[0]
    heads = key_ref.shape[2] // HEAD_SIZE
    sharing = query_ref.shape[1] // key_ref.shape[2]
    head_width = sharing * HEAD_SIZE
    columns = query_ref.shape[1]
    half = columns // 2
    blocks = WINDOW_LENGTH // shard_rows + 1

    barrier = pltpu.get_barrier_semaphore()
    for device in (ring.other, ring.ahead, ring.behind):
        pl.semaphore_signal(barrier, inc=1, device_id=(device, group), device_id_type=MESH)
    pl.semaphore_signal(barrier, inc=1, device_id=(me, 1 - group), device_id_type=MESH)

    def own_copy(source):
        return pltpu.make_async_copy(
            source, out_land.at[me // 2, :, pl.ds(core * columns, columns)], load_sem.at[0]
        )

    @pl.when(core == group)
    def _():
        own_copy(out_ref).start()

    @pl.when(core != group)
    def _():
        own_copy(swap_ref).start()

    def window_copies(slot):
        span = pl.ds(slot * shard_rows, shard_rows)
        copies = [
            pltpu.make_async_copy(key_ref.at[slot], key_window.at[span], load_sem.at[1 + slot])
        ]
        for head in range(heads):
            copies.append(
                pltpu.make_async_copy(
                    value_ref.at[slot, :, pl.ds(head * HEAD_SIZE, HEAD_SIZE)],
                    value_window.at[head, span, pl.ds(0, HEAD_SIZE)],
                    load_sem.at[1 + blocks + slot * heads + head],
                )
            )
        return copies

    for slot in range(blocks):
        distance = blocks - 1 - slot
        span = pl.ds(slot * shard_rows, shard_rows)

        @pl.when(me >= distance)
        def _():
            for copy in window_copies(slot):
                copy.start()
            for head in range(heads):
                value_window[head, span, pl.ds(HEAD_SIZE, HEAD_SIZE)] = jnp.ones(
                    (shard_rows, HEAD_SIZE), jnp.bfloat16
                )

        @pl.when(me < distance)
        def _():
            key_window[span, :] = jnp.zeros((shard_rows, key_window.shape[1]), jnp.bfloat16)
            for head in range(heads):
                value_window[head, span, :] = jnp.zeros(
                    (shard_rows, 2 * HEAD_SIZE), jnp.bfloat16
                )

    pl.semaphore_wait(barrier, 4)

    wide = half // pieces

    def flow(index, column, way):
        def slot_of(chip, side):
            start = pl.multiple_of(side * columns + column, 128)
            return out_land.at[chip, :, pl.ds(start, wide)]

        return index, slot_of, way

    flows = []
    for piece in range(pieces):
        flows.append(flow(2 * piece, piece * wide, 1))
        flows.append(flow(2 * piece + 1, half + piece * wide, -1))

    own_copy(out_ref).wait()
    ring.hop(flows, 0, first=True)

    for slot in range(blocks):
        distance = blocks - 1 - slot

        @pl.when(me >= distance)
        def _():
            for copy in window_copies(slot):
                copy.wait()

    tile = part_rows
    tiles = shard_rows // tile
    reach = WINDOW_LENGTH // tile
    lower = lax.broadcasted_iota(jnp.int32, (tile, tile), 1) > lax.broadcasted_iota(
        jnp.int32, (tile, tile), 0
    )
    masks = jnp.concatenate([lower] * sharing, axis=0)

    def place_of(unit):
        head, part = unit // tiles, unit % tiles
        start = pl.multiple_of(part * tile, tile)
        column = pl.multiple_of(head * head_width, HEAD_SIZE)
        return head, start, column

    def attend(unit):
        head, start, column = place_of(unit)
        stacked = jnp.concatenate(
            [
                query_ref[
                    pl.ds(start, tile),
                    pl.ds(pl.multiple_of(column + i * HEAD_SIZE, HEAD_SIZE), HEAD_SIZE),
                ]
                for i in range(sharing)
            ],
            axis=0,
        )
        key_columns = pl.ds(pl.multiple_of(head * HEAD_SIZE, HEAD_SIZE), HEAD_SIZE)

        def scores(index):
            keys = key_window[pl.ds(start + index * tile, tile), key_columns]
            return lax.dot_general(
                stacked, keys, (((1,), (1,)), ((), ())), preferred_element_type=jnp.float32
            )

        def mixed(index, weights):
            values = value_window[head, pl.ds(start + index * tile, tile), :]
            return jnp.dot(
                weights.astype(jnp.bfloat16), values, preferred_element_type=jnp.float32
            )

        edge = jnp.exp2(jnp.where(masks, scores(0), scores(reach)))
        total = mixed(0, jnp.where(masks, edge, 0.0))
        total = total + mixed(reach, jnp.where(masks, 0.0, edge))
        for index in range(1, reach):
            total = total + mixed(index, jnp.exp2(scores(index)))
        final = (total[:, :HEAD_SIZE] / total[:, HEAD_SIZE:]).astype(jnp.bfloat16)
        for i in range(sharing):
            attended[
                group,
                pl.ds(start, tile),
                pl.ds(pl.multiple_of(column + i * HEAD_SIZE, HEAD_SIZE), HEAD_SIZE),
            ] = final[i * tile : (i + 1) * tile]

    def mixed_copy(unit, side):
        _, start, column = place_of(unit)
        piece = attended.at[side, pl.ds(start, tile), pl.ds(column, head_width)]
        return pltpu.make_async_remote_copy(
            src_ref=piece,
            dst_ref=piece,
            send_sem=mixed_send.at[unit],
            recv_sem=mixed_recv.at[unit],
            device_id=(me, 1 - group),
            device_id_type=MESH,
        )

    units = heads * tiles

    def attend_step(unit, carry):
        attend(unit)

        @pl.when(unit > 0)
        def _():
            mixed_copy(unit - 1, group).start()

        return carry

    lax.fori_loop(0, units // 2, attend_step, 0)
    ring.hop(flows, 1)
    lax.fori_loop(units // 2, units, attend_step, 0)
    ring.hop(flows, 2)
    mixed_copy(units - 1, group).start()
    ring.hop(flows, 3)

    def received(unit, carry):
        mixed_copy(unit, 1 - group).wait_recv()
        return carry

    lax.fori_loop(0, units, received, 0)

    def back_copy(chip, side):
        return pltpu.make_async_remote_copy(
            src_ref=projected.at[chip, pl.ds(pl.multiple_of((1 - group) * part_rows, 16), part_rows)],
            dst_ref=gathered.at[side, chip],
            send_sem=back_send.at[chip],
            recv_sem=back_recv.at[chip],
            device_id=(me, 1 - group),
            device_id_type=MESH,
        )

    def project(way, step):
        chip = ring.owner(way, step)
        weights = out_land.at[chip]
        total = lax.dot_general(
            attended[0],
            weights[:, :columns],
            (((1,), (1,)), ((), ())),
            preferred_element_type=jnp.float32,
        )
        total = total + lax.dot_general(
            attended[1],
            weights[:, columns:],
            (((1,), (1,)), ((), ())),
            preferred_element_type=jnp.float32,
        )
        projected[chip] = total.astype(jnp.bfloat16)
        gathered[group, chip] = projected[
            chip, pl.ds(pl.multiple_of(group * part_rows, 16), part_rows)
        ]
        back_copy(chip, group).start()

    def landed(way, step):
        ring.landed([f for f in flows if f[2] == way], step)

    landed(1, 0)
    landed(-1, 0)
    project(1, 0)
    middle = chips // 2

    def early(step, carry):
        landed(1, step)
        landed(-1, step)
        return carry

    lax.fori_loop(1, 4, early, 0)

    def later(step, carry):
        ring.hop(flows, step)
        landed(1, step)
        landed(-1, step)

        @pl.when(step >= middle)
        def _():
            project(1, step)

            @pl.when(step > middle)
            def _():
                project(-1, step)

        return carry

    lax.fori_loop(4, chips - 1, later, 0)
    ring.hop(flows, chips - 1, last=True)
    landed(1, chips - 1)
    landed(-1, chips - 1)
    project(1, chips - 1)
    project(-1, chips - 1)

    def arrived(chip, carry):
        back_copy(chip, 1 - group).wait_recv()
        return carry

    lax.fori_loop(0, chips, arrived, 0)

    block = 16

    def final(index, carry):
        start = pl.multiple_of(index * block, block)
        values = jnp.concatenate(
            [
                gathered[side, chip, pl.ds(start, block), :].astype(jnp.float32)
                for chip in range(chips)
                for side in range(2)
            ],
            axis=1,
        )
        mean_square = jnp.mean(values * values, axis=-1, keepdims=True)
        scaled = values * lax.rsqrt(mean_square + epsilon) * gain_ref[...]
        rows = tokens_ref[pl.ds(start, block), :].astype(jnp.float32)
        result_ref[pl.ds(start, block), :] = (rows + scaled).astype(jnp.bfloat16)
        return carry

    lax.fori_loop(0, part_rows // block, final, 0)

    def sent(unit, carry):
        mixed_copy(unit, group).wait_send()
        return carry

    lax.fori_loop(0, units, sent, 0)

    def back_sent(chip, carry):
        back_copy(chip, group).wait_send()
        return carry

    lax.fori_loop(0, chips, back_sent, 0)
    ring.drain(flows)


def ring_semaphores(flows, chips):
    return [pltpu.SemaphoreType.DMA((flows, chips))] * 4


def on_device(
    tokens,
    norm_gain,
    query_weight,
    key_matrix,
    value_matrix,
    out_weight,
    query_gain,
    key_gain,
    post_gain,
):
    shards = lax.axis_size("seq")
    copies = lax.axis_size("fsdp")
    chips = shards // 2
    part_rows, model_width = tokens.shape
    shard_rows = part_rows * copies
    rows, query_width = query_weight.shape
    key_width = key_matrix.shape[1]
    merge = 2 if rows % 16 == 0 else 1
    blocks = WINDOW_LENGTH // shard_rows + 1

    positions = lax.axis_index("seq") * shard_rows + jnp.arange(shard_rows, dtype=jnp.int32)
    exponents = jnp.arange(HEAD_SIZE // 2, dtype=jnp.float32) * (2.0 / HEAD_SIZE)
    frequency = jnp.exp(-exponents * jnp.log(jnp.float32(rope_base)))
    angles = positions.astype(jnp.float32)[:, None] * frequency[None, :]
    cosine, sine = jnp.cos(angles), jnp.sin(angles)
    cosine = jnp.concatenate([cosine, cosine], axis=1)
    sine = jnp.concatenate([-sine, sine], axis=1)

    hbm = pl.BlockSpec(memory_space=pltpu.MemorySpace.HBM)
    vmem = pl.BlockSpec(memory_space=pltpu.VMEM)
    bf16, f32 = jnp.bfloat16, jnp.float32
    dma = pltpu.SemaphoreType.DMA
    stack = jax.ShapeDtypeStruct((blocks, shard_rows, key_width), bf16)
    queries, keys, values, swapped = pl.pallas_call(
        functools.partial(project_kernel, shards, merge),
        out_shape=[
            jax.ShapeDtypeStruct((shard_rows, query_width), bf16),
            stack,
            stack,
            jax.ShapeDtypeStruct(out_weight.shape, bf16),
        ],
        in_specs=[hbm, vmem, hbm, hbm, hbm, hbm, vmem, vmem, vmem, vmem],
        out_specs=[vmem, hbm, hbm, hbm],
        scratch_shapes=[
            pltpu.VMEM((shards, rows, query_width), bf16),
            pltpu.VMEM((shards, rows, key_width), bf16),
            pltpu.VMEM((shards, rows, key_width), bf16),
            pltpu.VMEM((copies, part_rows, model_width), bf16),
            pltpu.VMEM((shards // merge, shard_rows, merge * rows), bf16),
            pltpu.VMEM((shard_rows, query_width), f32),
            pltpu.VMEM((shard_rows, key_width), f32),
            pltpu.VMEM((shard_rows, key_width), f32),
            pltpu.VMEM((shard_rows, key_width), bf16),
            pltpu.VMEM((shard_rows, key_width), bf16),
            *ring_semaphores(4 * pieces, chips),
            dma((4,)),
            dma((token_pieces,)),
            dma((token_pieces,)),
            dma((2,)),
            dma((2,)),
            dma((2,)),
            dma((2,)),
            dma((2,)),
        ],
        compiler_params=pltpu.CompilerParams(
            collective_id=0, has_side_effects=True, vmem_limit_bytes=60 * 1024 * 1024
        ),
    )(
        tokens,
        norm_gain[None, :],
        query_weight,
        key_matrix,
        value_matrix,
        out_weight,
        query_gain[None, :],
        key_gain[None, :],
        cosine,
        sine,
    )
    heads = key_width // HEAD_SIZE
    units = heads * copies
    window = blocks * shard_rows
    return pl.pallas_call(
        functools.partial(attend_kernel, shards),
        out_shape=jax.ShapeDtypeStruct(tokens.shape, bf16),
        in_specs=[vmem, hbm, hbm, hbm, hbm, vmem, vmem],
        out_specs=vmem,
        scratch_shapes=[
            pltpu.VMEM((chips, rows, 2 * query_width), bf16),
            pltpu.VMEM((window, key_width), bf16),
            pltpu.VMEM((heads, window, 2 * HEAD_SIZE), bf16),
            pltpu.VMEM((copies, shard_rows, query_width), bf16),
            pltpu.VMEM((chips, shard_rows, rows), bf16),
            pltpu.VMEM((copies, chips, part_rows, rows), bf16),
            *ring_semaphores(2 * pieces, chips),
            dma((1 + blocks * (1 + heads),)),
            dma((units,)),
            dma((units,)),
            dma((chips,)),
            dma((chips,)),
        ],
        compiler_params=pltpu.CompilerParams(
            collective_id=1, has_side_effects=True, vmem_limit_bytes=60 * 1024 * 1024
        ),
    )(queries, keys, values, out_weight, swapped, tokens, post_gain[None, :])


def solution(mesh):
    in_specs = (
        P(("seq", "fsdp"), None),
        P(),
        P("seq", "fsdp"),
        P("seq", "fsdp"),
        P("seq", "fsdp"),
        P("seq", "fsdp"),
        P(),
        P(),
        P(),
    )
    out_specs = P(("seq", "fsdp"), None)
    return jax.shard_map(
        on_device, mesh=mesh, in_specs=in_specs, out_specs=out_specs, check_vma=False
    )
```

```python
import functools

import jax
import jax.numpy as jnp
from jax import lax
from jax.experimental import pallas as pl
from jax.experimental.pallas import tpu as pltpu
from jax.sharding import PartitionSpec as P

HEAD_SIZE = 128
WINDOW_LENGTH = 1024

epsilon = 1e-06
score_scale = 168.0 ** (-0.5)
log2_e = 1.4426950408889634
rope_base = 10000.0
pieces = 2
token_pieces = 4
MESH = pl.DeviceIdType.MESH


def ring_place(chip, chips):
    row, side = chip // 2, chip % 2
    return side * (chips - 1 - row) + (1 - side) * row


def ring_chip(place, chips):
    back = place // (chips // 2)
    return back * (2 * (chips - 1 - place) + 1) + (1 - back) * 2 * place


class Ring:
    def __init__(self, shards, sems):
        self.chips = shards // 2
        self.me = lax.axis_index("seq")
        self.group = lax.axis_index("fsdp")
        self.core = self.me % 2
        self.place = ring_place(self.me // 2, self.chips)
        self.other = (self.me // 2) * 2 + 1 - self.core
        self.ahead = self.neighbour(1)
        self.behind = self.neighbour(self.chips - 1)
        self.ring_send, self.ring_recv, self.pair_send, self.pair_recv = sems

    def neighbour(self, distance):
        return ring_chip((self.place + distance) % self.chips, self.chips) * 2 + self.core

    def owner(self, way, step):
        return ring_chip((self.place + (self.chips - way) * step) % self.chips, self.chips)

    def ring_copy(self, flow, step, sent):
        index, slot_of, way = flow
        slot = slot_of(self.owner(way, step), self.core)
        return pltpu.make_async_remote_copy(
            src_ref=slot,
            dst_ref=slot,
            send_sem=self.ring_send.at[index, sent],
            recv_sem=self.ring_recv.at[index, sent],
            device_id=(self.ahead if way > 0 else self.behind, self.group),
            device_id_type=MESH,
        )

    def pair_copy(self, flow, step, core):
        index, slot_of, way = flow
        slot = slot_of(self.owner(way, step), core)
        return pltpu.make_async_remote_copy(
            src_ref=slot,
            dst_ref=slot,
            send_sem=self.pair_send.at[index, step],
            recv_sem=self.pair_recv.at[index, step],
            device_id=(self.other, self.group),
            device_id_type=MESH,
        )

    def hop(self, step, flows, arrive=None, leave=None, hand=None):
        for flow in flows:
            if arrive is None or flow in arrive:
                self.ring_copy(flow, step, step - 1).wait_recv()
            if leave is None or flow in leave:
                self.ring_copy(flow, step, step).start()
            if hand is None or flow in hand:
                self.pair_copy(flow, step, self.core).start()

    def landed(self, flows, step):
        for flow in flows:
            self.pair_copy(flow, step, 1 - self.core).wait_recv()

    def sent(self, step, leave, hand):
        for flow in leave:
            self.ring_copy(flow, step, step).wait_send()
        for flow in hand:
            self.pair_copy(flow, step, self.core).wait_send()


def steps(first, last, body):
    def one(step, carry):
        body(step)
        return carry

    lax.fori_loop(first, last, one, 0)


def turned(values, gain, cosine, sine, scale):
    mean_square = jnp.mean(values * values, axis=-1, keepdims=True)
    normed = values * lax.rsqrt(mean_square + epsilon) * gain
    swapped = pltpu.roll(normed, values.shape[-1] // 2, 1)
    return (normed * cosine + swapped * sine) * scale


def layer_kernel(
    shards,
    merge,
    tokens_ref,
    gain_ref,
    query_ref,
    key_ref,
    value_ref,
    out_ref,
    query_gain_ref,
    key_gain_ref,
    post_gain_ref,
    cosine_ref,
    sine_ref,
    result_ref,
    swap_out,
    query_land,
    pair_land,
    raw,
    split,
    query_sum,
    key_sum,
    value_sum,
    queries,
    key_window,
    value_window,
    attended,
    projected,
    gathered,
    cosines,
    sines,
    ring_send,
    ring_recv,
    pair_send,
    pair_recv,
    local_sem,
    token_send,
    token_recv,
    swap_sem,
    far_send,
    far_recv,
    near_send,
    near_recv,
    mixed_send,
    mixed_recv,
    back_send,
    back_recv,
    free_sem,
):
    ring = Ring(shards, (ring_send, ring_recv, pair_send, pair_recv))
    chips, me, group, core = ring.chips, ring.me, ring.group, ring.core
    rows, width = key_ref.shape
    part_rows = tokens_ref.shape[0]
    columns = query_ref.shape[1]
    half = columns // 2
    shard_rows = queries.shape[0]
    heads = width // HEAD_SIZE
    query_heads = columns // HEAD_SIZE
    sharing = query_heads // heads
    head_width = sharing * HEAD_SIZE
    blocks = WINDOW_LENGTH // shard_rows + 1
    far_to = (me + 2) % shards
    far_from = (me + shards - 2) % shards
    middle = chips // 2

    barrier = pltpu.get_barrier_semaphore()
    for device in (ring.other, ring.ahead, ring.behind, far_to, far_from):
        pl.semaphore_signal(barrier, inc=1, device_id=(device, group), device_id_type=MESH)
    pl.semaphore_signal(barrier, inc=1, device_id=(me, 1 - group), device_id_type=MESH)

    @pl.when(core != group)
    def _():
        pl.semaphore_signal(
            barrier,
            inc=1,
            device_id=((me // 2) * 2 + group, core),
            device_id_type=MESH,
        )

    local = [
        pltpu.make_async_copy(key_ref, pair_land.at[me, :, pl.ds(0, width)], local_sem.at[0]),
        pltpu.make_async_copy(
            value_ref, pair_land.at[me, :, pl.ds(width, width)], local_sem.at[1]
        ),
        pltpu.make_async_copy(query_ref, query_land.at[me], local_sem.at[2]),
        pltpu.make_async_copy(tokens_ref, raw.at[group], local_sem.at[3]),
    ]
    for copy in local:
        copy.start()
    pl.semaphore_wait(barrier, 6 + (core + group) % 2)

    def flow(index, land, column, count, way):
        return index, lambda chip, side: land.at[chip * 2 + side, :, pl.ds(column, count)], way

    size, wide = width // pieces, half // pieces
    first, second = [], []
    for piece in range(pieces):
        first.append(flow(2 * piece, pair_land, piece * size, size, 1))
        first.append(flow(2 * piece + 1, pair_land, width + piece * size, size, -1))
    for piece in range(pieces):
        base = 2 * (pieces + piece)
        second.append(flow(base, query_land, piece * wide, wide, 1))
        second.append(flow(base + 1, query_land, half + piece * wide, wide, -1))
    third = []
    for piece in range(2):
        for way in (1, -1):
            third.append(flow(4 * pieces + len(third), pair_land, piece * half, half, way))
    origin = [third[0], third[2]]
    farthest = [third[0], third[3]]

    token_rows = part_rows // token_pieces

    def token_copy(piece, side):
        span = pl.ds(piece * token_rows, token_rows)
        return pltpu.make_async_remote_copy(
            src_ref=tokens_ref.at[span],
            dst_ref=raw.at[side, span],
            send_sem=token_send.at[piece],
            recv_sem=token_recv.at[piece],
            device_id=(me, 1 - group),
            device_id_type=MESH,
        )

    swap = pltpu.make_async_remote_copy(
        src_ref=out_ref,
        dst_ref=swap_out,
        send_sem=swap_sem.at[0],
        recv_sem=swap_sem.at[1],
        device_id=((me // 2) * 2 + group, core),
        device_id_type=MESH,
    )

    local[0].wait()
    local[1].wait()
    ring.hop(0, first, arrive=[])
    for piece in range(token_pieces):
        token_copy(piece, group).start()

    @pl.when(core != group)
    def _():
        swap.start()

    local[2].wait()
    local[3].wait()

    block = 16
    span_width = rows * merge

    def normed_rows(side, begin, count):
        def one(index):
            start = pl.multiple_of(begin + index * block, block)
            values = raw[side, pl.ds(start, block), :].astype(jnp.float32)
            mean_square = jnp.mean(values * values, axis=-1, keepdims=True)
            normed = values * lax.rsqrt(mean_square + epsilon) * gain_ref[...][None, :]
            target = pl.multiple_of(side * part_rows + start, block)
            for part in range(shards // merge):
                piece = normed[:, part * span_width : (part + 1) * span_width]
                split[part, pl.ds(target, block), :] = piece.astype(jnp.bfloat16)

        steps(0, count // block, one)

    normed_rows(group, 0, part_rows)
    key_sum[...] = jnp.zeros_like(key_sum)
    value_sum[...] = jnp.zeros_like(value_sum)
    query_sum[...] = jnp.zeros_like(query_sum)
    cosines[...] = jnp.concatenate([cosine_ref[...], cosine_ref[...]], axis=1)
    sines[...] = jnp.concatenate([-sine_ref[...], sine_ref[...]], axis=1)

    for slot in range(blocks - 1):
        distance = blocks - 1 - slot
        span = pl.ds(slot * shard_rows, shard_rows)

        @pl.when(me < distance)
        def _():
            key_window[span, :] = jnp.zeros((shard_rows, width), jnp.bfloat16)
            for head in range(heads):
                value_window[head, span, :] = jnp.zeros(
                    (shard_rows, 2 * HEAD_SIZE), jnp.bfloat16
                )

    for slot in range(blocks):
        span = pl.ds(slot * shard_rows, shard_rows)

        @pl.when(me >= blocks - 1 - slot)
        def _():
            for head in range(heads):
                value_window[head, span, pl.ds(HEAD_SIZE, HEAD_SIZE)] = jnp.ones(
                    (shard_rows, HEAD_SIZE), jnp.bfloat16
                )

    def products(total, begin, land, column, count, chip):
        target = pl.ds(begin, count)
        taken = pl.ds(column, count)
        if merge == 2:
            weights = land[pl.ds(chip * 2, 2), :, taken].reshape(2 * rows, count)
            total[:, target] += jnp.dot(
                split[chip], weights, preferred_element_type=jnp.float32
            )
        else:
            for side in range(2):
                total[:, target] += jnp.dot(
                    split[chip * 2 + side],
                    land[chip * 2 + side, :, taken],
                    preferred_element_type=jnp.float32,
                )

    def key_value(step):
        products(key_sum, 0, pair_land, 0, width, ring.owner(1, step))
        products(value_sum, 0, pair_land, width, width, ring.owner(-1, step))

    def query(step):
        products(query_sum, 0, query_land, 0, half, ring.owner(1, step))
        products(query_sum, half, query_land, half, half, ring.owner(-1, step))

    steps(1, chips - 1, lambda step: ring.hop(step, first))
    ring.hop(0, second, arrive=[])
    ring.hop(chips - 1, first, leave=[])
    for piece in range(token_pieces - 1):
        token_copy(piece, 1 - group).wait_recv()
    normed_rows(1 - group, 0, part_rows - token_rows)
    steps(0, chips, lambda step: ring.landed(first, step))

    def span_of(slot):
        return pl.ds(slot * shard_rows, shard_rows)

    def key_part(slot):
        return key_window.at[span_of(slot)]

    def value_part(slot):
        return value_window.at[:, span_of(slot), pl.ds(0, HEAD_SIZE)]

    stacks = ((0, key_part), (1, value_part))

    def far_copy(index, part):
        return pltpu.make_async_remote_copy(
            src_ref=part(blocks - 1),
            dst_ref=part(0),
            send_sem=far_send.at[index],
            recv_sem=far_recv.at[index],
            device_id=(far_to, group),
            device_id_type=MESH,
        )

    def near_copy(index, part, slot):
        return pltpu.make_async_remote_copy(
            src_ref=part(slot),
            dst_ref=part(1),
            send_sem=near_send.at[index],
            recv_sem=near_recv.at[index],
            device_id=(ring.other, group),
            device_id_type=MESH,
        )

    def head_columns(head):
        return pl.ds(pl.multiple_of(head * HEAD_SIZE, HEAD_SIZE), HEAD_SIZE)

    def finish_keys():
        def one(head):
            taken = head_columns(head)
            key_window[span_of(blocks - 1), taken] = turned(
                key_sum[:, taken], key_gain_ref[...][None, :], cosines[...], sines[...], 1.0
            ).astype(jnp.bfloat16)
            value_window[head, span_of(blocks - 1), pl.ds(0, HEAD_SIZE)] = value_sum[
                :, taken
            ].astype(jnp.bfloat16)

        steps(0, heads, one)

    def send_keys():
        for index, part in stacks:

            @pl.when(me + 2 < shards)
            def _():
                far_copy(index, part).start()

            @pl.when(core == 0)
            def _():
                near_copy(index, part, blocks - 1).start()

    def own_copy(source):
        return pltpu.make_async_copy(source, pair_land.at[me], local_sem.at[0])

    def free_slots():
        steps(0, chips - 1, lambda step: ring.sent(step, first, first))
        ring.sent(chips - 1, [], first)
        for device in (ring.other, ring.ahead, ring.behind):
            pl.semaphore_signal(
                free_sem, inc=1, device_id=(device, group), device_id_type=MESH
            )

        @pl.when(core == group)
        def _():
            own_copy(out_ref).start()

        @pl.when(core != group)
        def _():
            swap.wait()
            own_copy(swap_out).start()

    def second_step(step):
        ring.hop(step, second)
        ring.landed(second, step - 1)

        @pl.when(step == 1)
        def _():
            token_copy(token_pieces - 1, 1 - group).wait_recv()
            normed_rows(1 - group, part_rows - token_rows, token_rows)
            steps(0, middle, key_value)

        @pl.when(step == 2)
        def _():
            steps(middle, chips, key_value)
            finish_keys()

        @pl.when(step == 3)
        def _():
            query(0)
            send_keys()
            steps(1, 3, query)

        @pl.when(step > 3)
        def _():
            query(step - 1)

        @pl.when(step == 4)
        def _():
            free_slots()

    steps(1, chips - 1, second_step)

    pl.semaphore_wait(free_sem, 3)
    own_copy(out_ref).wait()
    ring.hop(0, third, arrive=[], hand=origin)
    ring.hop(chips - 1, second, leave=[])
    ring.landed(second, chips - 2)
    query(chips - 2)

    @pl.when(me >= 2)
    def _():
        for index, part in stacks:
            far_copy(index, part).wait_recv()

            @pl.when(core == 1)
            def _():
                near_copy(index, part, 0).start()

    ring.landed(second, chips - 1)
    query(chips - 1)

    def finish_query(head):
        taken = head_columns(head)
        queries[:, taken] = turned(
            query_sum[:, taken],
            query_gain_ref[...][None, :],
            cosines[...],
            sines[...],
            score_scale * log2_e,
        ).astype(jnp.bfloat16)

    steps(0, query_heads, finish_query)

    for index, part in stacks:

        @pl.when(core == 1)
        def _():
            near_copy(index, part, 0).wait_recv()

        @pl.when(core == 0)
        def _():
            @pl.when(me >= 2)
            def _():
                near_copy(index, part, 0).wait_recv()

    tile = part_rows
    tiles = shard_rows // tile
    reach = WINDOW_LENGTH // tile
    lower = lax.broadcasted_iota(jnp.int32, (tile, tile), 1) > lax.broadcasted_iota(
        jnp.int32, (tile, tile), 0
    )
    masks = jnp.concatenate([lower] * sharing, axis=0)

    def place_of(unit):
        head, part = unit // tiles, unit % tiles
        start = pl.multiple_of(part * tile, tile)
        column = pl.multiple_of(head * head_width, HEAD_SIZE)
        return head, start, column

    def attend(unit):
        head, start, column = place_of(unit)
        taken = [
            pl.ds(pl.multiple_of(column + i * HEAD_SIZE, HEAD_SIZE), HEAD_SIZE)
            for i in range(sharing)
        ]
        stacked = jnp.concatenate([queries[pl.ds(start, tile), c] for c in taken], axis=0)
        key_columns = head_columns(head)

        def scores(index):
            keys = key_window[pl.ds(start + index * tile, tile), key_columns]
            return lax.dot_general(
                stacked, keys, (((1,), (1,)), ((), ())), preferred_element_type=jnp.float32
            )

        def mixed(index, weights):
            values = value_window[head, pl.ds(start + index * tile, tile), :]
            return jnp.dot(
                weights.astype(jnp.bfloat16), values, preferred_element_type=jnp.float32
            )

        edge = jnp.exp2(jnp.where(masks, scores(0), scores(reach)))
        total = mixed(0, jnp.where(masks, edge, 0.0))
        total = total + mixed(reach, jnp.where(masks, 0.0, edge))
        for index in range(1, reach):
            total = total + mixed(index, jnp.exp2(scores(index)))
        final = (total[:, :HEAD_SIZE] / total[:, HEAD_SIZE:]).astype(jnp.bfloat16)
        for i in range(sharing):
            attended[group, pl.ds(start, tile), taken[i]] = final[i * tile : (i + 1) * tile]

    def mixed_copy(unit, side):
        _, start, column = place_of(unit)
        piece = attended.at[side, pl.ds(start, tile), pl.ds(column, head_width)]
        return pltpu.make_async_remote_copy(
            src_ref=piece,
            dst_ref=piece,
            send_sem=mixed_send.at[unit],
            recv_sem=mixed_recv.at[unit],
            device_id=(me, 1 - group),
            device_id_type=MESH,
        )

    units = heads * tiles

    def attend_step(unit):
        attend(unit)

        @pl.when(unit > 0)
        def _():
            mixed_copy(unit - 1, group).start()

    def back_copy(chip, side):
        away = pl.multiple_of((1 - group) * part_rows, 16)
        return pltpu.make_async_remote_copy(
            src_ref=projected.at[chip, pl.ds(away, part_rows)],
            dst_ref=gathered.at[side, chip],
            send_sem=back_send.at[chip],
            recv_sem=back_recv.at[chip],
            device_id=(me, 1 - group),
            device_id_type=MESH,
        )

    def project(way, step):
        chip = ring.owner(way, step)
        parts = [
            lax.dot_general(
                attended[side],
                pair_land[chip * 2 + side],
                (((1,), (1,)), ((), ())),
                preferred_element_type=jnp.float32,
            )
            for side in range(2)
        ]
        projected[chip] = (parts[0] + parts[1]).astype(jnp.bfloat16)
        home = pl.multiple_of(group * part_rows, 16)
        gathered[group, chip] = projected[chip, pl.ds(home, part_rows)]
        back_copy(chip, group).start()

    steps(0, units, attend_step)
    ring.hop(1, third)
    mixed_copy(units - 1, group).start()
    steps(0, units, lambda unit: mixed_copy(unit, 1 - group).wait_recv())
    ring.landed(origin, 0)
    project(1, 0)

    def both(step):
        ring.landed(third, step)
        project(1, step)
        project(-1, step)

    def third_step(step):
        both(step - 1)
        ring.hop(step, third)

    steps(2, middle - 1, third_step)
    both(middle - 2)
    ring.hop(middle - 1, third, leave=farthest)
    both(middle - 1)
    ring.hop(middle, farthest, leave=[])
    ring.landed(farthest, middle)
    project(1, middle)
    steps(0, chips, lambda chip: back_copy(chip, 1 - group).wait_recv())

    def final(index):
        start = pl.multiple_of(index * block, block)
        values = jnp.concatenate(
            [
                gathered[side, chip, pl.ds(start, block), :].astype(jnp.float32)
                for chip in range(chips)
                for side in range(2)
            ],
            axis=1,
        )
        mean_square = jnp.mean(values * values, axis=-1, keepdims=True)
        scaled = values * lax.rsqrt(mean_square + epsilon) * post_gain_ref[...][None, :]
        added = raw[group, pl.ds(start, block), :].astype(jnp.float32) + scaled
        result_ref[pl.ds(start, block), :] = added.astype(jnp.bfloat16)

    steps(0, part_rows // block, final)

    for index, part in stacks:

        @pl.when(me + 2 < shards)
        def _():
            far_copy(index, part).wait_send()

        @pl.when(core == 0)
        def _():
            near_copy(index, part, blocks - 1).wait_send()

        @pl.when(core == 1)
        def _():
            @pl.when(me >= 2)
            def _():
                near_copy(index, part, 0).wait_send()

    for piece in range(token_pieces):
        token_copy(piece, group).wait_send()
    steps(0, chips - 1, lambda step: ring.sent(step, second, second))
    ring.sent(chips - 1, [], second)
    ring.sent(0, third, origin)
    steps(1, middle - 1, lambda step: ring.sent(step, third, third))
    ring.sent(middle - 1, farthest, third)
    ring.sent(middle, [], farthest)
    steps(0, units, lambda unit: mixed_copy(unit, group).wait_send())
    steps(0, chips, lambda chip: back_copy(chip, group).wait_send())


def on_device(
    tokens,
    norm_gain,
    query_weight,
    key_matrix,
    value_matrix,
    out_weight,
    query_gain,
    key_gain,
    post_gain,
):
    shards = lax.axis_size("seq")
    copies = lax.axis_size("fsdp")
    chips = shards // 2
    part_rows, model_width = tokens.shape
    shard_rows = part_rows * copies
    rows, query_width = query_weight.shape
    key_width = key_matrix.shape[1]
    merge = 2 if rows % 16 == 0 else 1
    heads = key_width // HEAD_SIZE
    units = heads * copies
    window = WINDOW_LENGTH + shard_rows

    positions = lax.axis_index("seq") * shard_rows + jnp.arange(shard_rows, dtype=jnp.int32)
    exponents = jnp.arange(HEAD_SIZE // 2, dtype=jnp.float32) * (2.0 / HEAD_SIZE)
    frequency = jnp.exp(-exponents * jnp.log(jnp.float32(rope_base)))
    angles = positions.astype(jnp.float32)[:, None] * frequency[None, :]

    hbm = pl.BlockSpec(memory_space=pltpu.MemorySpace.HBM)
    vmem = pl.BlockSpec(memory_space=pltpu.VMEM)
    bf16, f32 = jnp.bfloat16, jnp.float32
    dma = pltpu.SemaphoreType.DMA
    result, _ = pl.pallas_call(
        functools.partial(layer_kernel, shards, merge),
        out_shape=[
            jax.ShapeDtypeStruct(tokens.shape, bf16),
            jax.ShapeDtypeStruct(out_weight.shape, bf16),
        ],
        in_specs=[hbm, vmem, hbm, hbm, hbm, hbm, vmem, vmem, vmem, vmem, vmem],
        out_specs=[vmem, hbm],
        scratch_shapes=[
            pltpu.VMEM((shards, rows, query_width), bf16),
            pltpu.VMEM((shards, rows, query_width), bf16),
            pltpu.VMEM((copies, part_rows, model_width), bf16),
            pltpu.VMEM((shards // merge, shard_rows, merge * rows), bf16),
            pltpu.VMEM((shard_rows, query_width), f32),
            pltpu.VMEM((shard_rows, key_width), f32),
            pltpu.VMEM((shard_rows, key_width), f32),
            pltpu.VMEM((shard_rows, query_width), bf16),
            pltpu.VMEM((window, key_width), bf16),
            pltpu.VMEM((heads, window, 2 * HEAD_SIZE), bf16),
            pltpu.VMEM((copies, shard_rows, query_width), bf16),
            pltpu.VMEM((chips, shard_rows, rows), bf16),
            pltpu.VMEM((copies, chips, part_rows, rows), bf16),
            pltpu.VMEM((shard_rows, HEAD_SIZE), f32),
            pltpu.VMEM((shard_rows, HEAD_SIZE), f32),
            *[dma((4 * pieces + 4, chips))] * 4,
            dma((4,)),
            dma((token_pieces,)),
            dma((token_pieces,)),
            dma((2,)),
            dma((2,)),
            dma((2,)),
            dma((2,)),
            dma((2,)),
            dma((units,)),
            dma((units,)),
            dma((chips,)),
            dma((chips,)),
            pltpu.SemaphoreType.REGULAR,
        ],
        compiler_params=pltpu.CompilerParams(
            collective_id=0, has_side_effects=True, vmem_limit_bytes=67043328
        ),
    )(
        tokens,
        norm_gain,
        query_weight,
        key_matrix,
        value_matrix,
        out_weight,
        query_gain,
        key_gain,
        post_gain,
        jnp.cos(angles),
        jnp.sin(angles),
    )
    return result


def solution(mesh):
    in_specs = (
        P(("seq", "fsdp"), None),
        P(),
        P("seq", "fsdp"),
        P("seq", "fsdp"),
        P("seq", "fsdp"),
        P("seq", "fsdp"),
        P(),
        P(),
        P(),
    )
    out_specs = P(("seq", "fsdp"), None)
    return jax.shard_map(
        on_device, mesh=mesh, in_specs=in_specs, out_specs=out_specs, check_vma=False
    )
```

```python
import functools
import math

import jax
import jax.numpy as jnp
from jax import lax
from jax.experimental import pallas as pl
from jax.experimental.pallas import tpu as pltpu
from jax.sharding import PartitionSpec as P

HEAD_SIZE = 128
WINDOW_LENGTH = 1024

epsilon = 1e-06
score_scale = 168.0 ** (-0.5)
log2_e = 1.4426950408889634
rope_base = 10000.0
pieces = 2
token_pieces = 4
MESH = pl.DeviceIdType.MESH


def ring_place(chip, chips):
    row, side = chip // 2, chip % 2
    return side * (chips - 1 - row) + (1 - side) * row


def ring_chip(place, chips):
    back = place // (chips // 2)
    return back * (2 * (chips - 1 - place) + 1) + (1 - back) * 2 * place


class Ring:
    def __init__(self, shards, sems):
        self.chips = shards // 2
        self.me = lax.axis_index("seq")
        self.group = lax.axis_index("fsdp")
        self.core = self.me % 2
        self.place = ring_place(self.me // 2, self.chips)
        self.other = (self.me // 2) * 2 + 1 - self.core
        self.ahead = self.neighbour(1)
        self.behind = self.neighbour(self.chips - 1)
        self.ring_send, self.ring_recv, self.pair_send, self.pair_recv = sems

    def neighbour(self, distance):
        return ring_chip((self.place + distance) % self.chips, self.chips) * 2 + self.core

    def owner(self, way, step):
        return ring_chip((self.place + (self.chips - way) * step) % self.chips, self.chips)

    def ring_copy(self, flow, step, sent):
        index, slot_of, way = flow
        slot = slot_of(self.owner(way, step), self.core)
        return pltpu.make_async_remote_copy(
            src_ref=slot,
            dst_ref=slot,
            send_sem=self.ring_send.at[index, sent],
            recv_sem=self.ring_recv.at[index, sent],
            device_id=(self.ahead if way > 0 else self.behind, self.group),
            device_id_type=MESH,
        )

    def pair_copy(self, flow, step, core):
        index, slot_of, way = flow
        slot = slot_of(self.owner(way, step), core)
        return pltpu.make_async_remote_copy(
            src_ref=slot,
            dst_ref=slot,
            send_sem=self.pair_send.at[index, step],
            recv_sem=self.pair_recv.at[index, step],
            device_id=(self.other, self.group),
            device_id_type=MESH,
        )

    def hop(self, step, flows, arrive=None, leave=None, hand=None):
        for flow in flows:
            if arrive is None or flow in arrive:
                self.ring_copy(flow, step, step - 1).wait_recv()
            if leave is None or flow in leave:
                self.ring_copy(flow, step, step).start()
            if hand is None or flow in hand:
                self.pair_copy(flow, step, self.core).start()

    def landed(self, flows, step):
        for flow in flows:
            self.pair_copy(flow, step, 1 - self.core).wait_recv()

    def sent(self, step, leave, hand):
        for flow in leave:
            self.ring_copy(flow, step, step).wait_send()
        for flow in hand:
            self.pair_copy(flow, step, self.core).wait_send()


def steps(first, last, body):
    def one(step, carry):
        body(step)
        return carry

    lax.fori_loop(first, last, one, 0)


def turned(values, gain, cosine, sine, scale):
    mean_square = jnp.mean(values * values, axis=-1, keepdims=True)
    normed = values * lax.rsqrt(mean_square + epsilon) * gain
    swapped = pltpu.roll(normed, values.shape[-1] // 2, 1)
    return (normed * cosine + swapped * sine) * scale


def layer_kernel(
    shards,
    merge,
    tokens_ref,
    gain_ref,
    query_ref,
    key_ref,
    value_ref,
    out_ref,
    query_gain_ref,
    key_gain_ref,
    gathered,
    swap_out,
    query_land,
    pair_land,
    raw,
    split,
    query_sum,
    key_sum,
    value_sum,
    queries,
    key_window,
    value_window,
    attended,
    projected,
    cosines,
    sines,
    ring_send,
    ring_recv,
    pair_send,
    pair_recv,
    local_sem,
    token_send,
    token_recv,
    swap_sem,
    far_send,
    far_recv,
    near_send,
    near_recv,
    mixed_send,
    mixed_recv,
    back_send,
    back_recv,
    home_sem,
    free_sem,
):
    ring = Ring(shards, (ring_send, ring_recv, pair_send, pair_recv))
    chips, me, group, core = ring.chips, ring.me, ring.group, ring.core
    rows, width = key_ref.shape
    part_rows = tokens_ref.shape[0]
    columns = query_ref.shape[1]
    half = columns // 2
    shard_rows = queries.shape[0]
    heads = width // HEAD_SIZE
    query_heads = columns // HEAD_SIZE
    sharing = query_heads // heads
    head_width = sharing * HEAD_SIZE
    blocks = WINDOW_LENGTH // shard_rows + 1
    far_to = (me + 2) % shards
    far_from = (me + shards - 2) % shards
    middle = chips // 2

    barrier = pltpu.get_barrier_semaphore()
    for device in (ring.other, ring.ahead, ring.behind, far_to, far_from):
        pl.semaphore_signal(barrier, inc=1, device_id=(device, group), device_id_type=MESH)
    pl.semaphore_signal(barrier, inc=1, device_id=(me, 1 - group), device_id_type=MESH)

    @pl.when(core != group)
    def _():
        pl.semaphore_signal(
            barrier,
            inc=1,
            device_id=((me // 2) * 2 + group, core),
            device_id_type=MESH,
        )

    local = [
        pltpu.make_async_copy(key_ref, pair_land.at[me, :, pl.ds(0, width)], local_sem.at[0]),
        pltpu.make_async_copy(
            value_ref, pair_land.at[me, :, pl.ds(width, width)], local_sem.at[1]
        ),
        pltpu.make_async_copy(query_ref, query_land.at[me], local_sem.at[2]),
        pltpu.make_async_copy(tokens_ref, raw.at[group], local_sem.at[3]),
    ]
    for copy in local:
        copy.start()
    pl.semaphore_wait(barrier, 6 + (core + group) % 2)

    def flow(index, land, column, count, way):
        return index, lambda chip, side: land.at[chip * 2 + side, :, pl.ds(column, count)], way

    size, wide = width // pieces, half // pieces
    first, second = [], []
    for piece in range(pieces):
        first.append(flow(2 * piece, pair_land, piece * size, size, 1))
        first.append(flow(2 * piece + 1, pair_land, width + piece * size, size, -1))
    for piece in range(pieces):
        base = 2 * (pieces + piece)
        second.append(flow(base, query_land, piece * wide, wide, 1))
        second.append(flow(base + 1, query_land, half + piece * wide, wide, -1))
    third = []
    for piece in range(2):
        for way in (1, -1):
            third.append(flow(4 * pieces + len(third), pair_land, piece * half, half, way))
    origin = [third[0], third[2]]
    farthest = [third[0], third[3]]

    token_rows = part_rows // token_pieces

    def token_copy(piece, side):
        span = pl.ds(piece * token_rows, token_rows)
        return pltpu.make_async_remote_copy(
            src_ref=tokens_ref.at[span],
            dst_ref=raw.at[side, span],
            send_sem=token_send.at[piece],
            recv_sem=token_recv.at[piece],
            device_id=(me, 1 - group),
            device_id_type=MESH,
        )

    swap = pltpu.make_async_remote_copy(
        src_ref=out_ref,
        dst_ref=swap_out,
        send_sem=swap_sem.at[0],
        recv_sem=swap_sem.at[1],
        device_id=((me // 2) * 2 + group, core),
        device_id_type=MESH,
    )

    local[0].wait()
    local[1].wait()
    ring.hop(0, first, arrive=[])
    for piece in range(token_pieces):
        token_copy(piece, group).start()

    @pl.when(core != group)
    def _():
        swap.start()

    local[2].wait()
    local[3].wait()

    block = 16
    span_width = rows * merge

    def normed_rows(side, begin, count):
        def one(index):
            start = pl.multiple_of(begin + index * block, block)
            values = raw[side, pl.ds(start, block), :].astype(jnp.float32)
            mean_square = jnp.mean(values * values, axis=-1, keepdims=True)
            normed = values * lax.rsqrt(mean_square + epsilon) * gain_ref[...][None, :]
            target = pl.multiple_of(side * part_rows + start, block)
            for part in range(shards // merge):
                piece = normed[:, part * span_width : (part + 1) * span_width]
                split[part, pl.ds(target, block), :] = piece.astype(jnp.bfloat16)

        steps(0, count // block, one)

    normed_rows(group, 0, part_rows)
    key_sum[...] = jnp.zeros_like(key_sum)
    value_sum[...] = jnp.zeros_like(value_sum)
    query_sum[...] = jnp.zeros_like(query_sum)
    lanes = lax.broadcasted_iota(jnp.int32, (shard_rows, HEAD_SIZE), 1)
    positions = me * shard_rows + lax.broadcasted_iota(jnp.int32, (shard_rows, HEAD_SIZE), 0)
    exponents = (lanes % (HEAD_SIZE // 2)).astype(jnp.float32) * (2.0 / HEAD_SIZE)
    angles = positions.astype(jnp.float32) * jnp.exp(-exponents * math.log(rope_base))
    cosines[...] = jnp.cos(angles)
    turn = jnp.sin(angles)
    sines[...] = jnp.where(lanes < HEAD_SIZE // 2, -turn, turn)

    for slot in range(blocks - 1):
        distance = blocks - 1 - slot
        span = pl.ds(slot * shard_rows, shard_rows)

        @pl.when(me < distance)
        def _():
            key_window[span, :] = jnp.zeros((shard_rows, width), jnp.bfloat16)
            for head in range(heads):
                value_window[head, span, :] = jnp.zeros(
                    (shard_rows, 2 * HEAD_SIZE), jnp.bfloat16
                )

    for slot in range(blocks):
        span = pl.ds(slot * shard_rows, shard_rows)

        @pl.when(me >= blocks - 1 - slot)
        def _():
            for head in range(heads):
                value_window[head, span, pl.ds(HEAD_SIZE, HEAD_SIZE)] = jnp.ones(
                    (shard_rows, HEAD_SIZE), jnp.bfloat16
                )

    def products(total, begin, land, column, count, chip):
        target = pl.ds(begin, count)
        taken = pl.ds(column, count)
        if merge == 2:
            weights = land[pl.ds(chip * 2, 2), :, taken].reshape(2 * rows, count)
            total[:, target] += jnp.dot(
                split[chip], weights, preferred_element_type=jnp.float32
            )
        else:
            for side in range(2):
                total[:, target] += jnp.dot(
                    split[chip * 2 + side],
                    land[chip * 2 + side, :, taken],
                    preferred_element_type=jnp.float32,
                )

    def key_value(step):
        products(key_sum, 0, pair_land, 0, width, ring.owner(1, step))
        products(value_sum, 0, pair_land, width, width, ring.owner(-1, step))

    def query(flows, step):
        column = flows[0][0] // 2 % pieces * wide
        ring.landed(flows, step)
        products(query_sum, column, query_land, column, wide, ring.owner(1, step))
        column += half
        products(query_sum, column, query_land, column, wide, ring.owner(-1, step))

    early, late = second[:2], second[2:]

    steps(1, chips - 3, lambda step: ring.hop(step, first))
    ring.hop(chips - 3, first)
    ring.hop(0, early, arrive=[])
    ring.hop(chips - 2, first)
    ring.hop(1, early)
    ring.hop(0, late, arrive=[])
    ring.hop(chips - 1, first, leave=[])
    ring.hop(2, early)
    for piece in range(token_pieces - 1):
        token_copy(piece, 1 - group).wait_recv()
    normed_rows(1 - group, 0, part_rows - token_rows)
    steps(0, chips, lambda step: ring.landed(first, step))

    def span_of(slot):
        return pl.ds(slot * shard_rows, shard_rows)

    def key_part(slot):
        return key_window.at[span_of(slot)]

    def value_part(slot):
        return value_window.at[:, span_of(slot), pl.ds(0, HEAD_SIZE)]

    stacks = ((0, key_part), (1, value_part))

    def far_copy(index, part):
        return pltpu.make_async_remote_copy(
            src_ref=part(blocks - 1),
            dst_ref=part(0),
            send_sem=far_send.at[index],
            recv_sem=far_recv.at[index],
            device_id=(far_to, group),
            device_id_type=MESH,
        )

    def near_copy(index, part, slot):
        return pltpu.make_async_remote_copy(
            src_ref=part(slot),
            dst_ref=part(1),
            send_sem=near_send.at[index],
            recv_sem=near_recv.at[index],
            device_id=(ring.other, group),
            device_id_type=MESH,
        )

    def head_columns(head):
        return pl.ds(pl.multiple_of(head * HEAD_SIZE, HEAD_SIZE), HEAD_SIZE)

    def finish_keys():
        def one(head):
            taken = head_columns(head)
            key_window[span_of(blocks - 1), taken] = turned(
                key_sum[:, taken], key_gain_ref[...][None, :], cosines[...], sines[...], 1.0
            ).astype(jnp.bfloat16)
            value_window[head, span_of(blocks - 1), pl.ds(0, HEAD_SIZE)] = value_sum[
                :, taken
            ].astype(jnp.bfloat16)

        steps(0, heads, one)

    def send_keys():
        for index, part in stacks:

            @pl.when(me + 2 < shards)
            def _():
                far_copy(index, part).start()

            @pl.when(core == 0)
            def _():
                near_copy(index, part, blocks - 1).start()

    def own_copy(source):
        return pltpu.make_async_copy(source, pair_land.at[me], local_sem.at[0])

    def free_slots():
        steps(0, chips - 1, lambda step: ring.sent(step, first, first))
        ring.sent(chips - 1, [], first)
        for device in (ring.other, ring.ahead, ring.behind):
            pl.semaphore_signal(
                free_sem, inc=1, device_id=(device, group), device_id_type=MESH
            )

        @pl.when(core == group)
        def _():
            own_copy(out_ref).start()

        @pl.when(core != group)
        def _():
            swap.wait()
            own_copy(swap_out).start()

    def second_step(step):
        ring.hop(step + 2, early)
        ring.hop(step, late)

        @pl.when(step == 1)
        def _():
            token_copy(token_pieces - 1, 1 - group).wait_recv()
            normed_rows(1 - group, part_rows - token_rows, token_rows)
            steps(0, middle, key_value)

        @pl.when(step == 2)
        def _():
            steps(middle, chips, key_value)
            finish_keys()

        @pl.when(step == 3)
        def _():
            query(early, 0)
            send_keys()
            steps(1, 5, lambda step: query(early, step))
            steps(0, 3, lambda step: query(late, step))

        @pl.when(step > 3)
        def _():
            query(early, step + 1)
            query(late, step - 1)

        @pl.when(step == 4)
        def _():
            free_slots()

    def finish_query(column):
        def one(head):
            taken = pl.ds(pl.multiple_of(column + head * HEAD_SIZE, HEAD_SIZE), HEAD_SIZE)
            queries[:, taken] = turned(
                query_sum[:, taken],
                query_gain_ref[...][None, :],
                cosines[...],
                sines[...],
                score_scale * log2_e,
            ).astype(jnp.bfloat16)

        steps(0, wide // HEAD_SIZE, one)

    steps(1, chips - 3, second_step)
    ring.hop(chips - 1, early, leave=[])
    ring.hop(chips - 3, late)
    query(early, chips - 2)
    query(late, chips - 4)
    query(early, chips - 1)
    finish_query(0)
    finish_query(half)
    ring.hop(chips - 2, late)
    pl.semaphore_wait(free_sem, 3)
    own_copy(out_ref).wait()
    ring.hop(0, third, arrive=[], hand=origin)
    query(late, chips - 3)

    @pl.when(me >= 2)
    def _():
        for index, part in stacks:
            far_copy(index, part).wait_recv()

            @pl.when(core == 1)
            def _():
                near_copy(index, part, 0).start()

    for index, part in stacks:

        @pl.when(core == 1)
        def _():
            near_copy(index, part, 0).wait_recv()

        @pl.when(core == 0)
        def _():
            @pl.when(me >= 2)
            def _():
                near_copy(index, part, 0).wait_recv()

    tile = part_rows
    tiles = shard_rows // tile
    reach = WINDOW_LENGTH // tile
    lower = lax.broadcasted_iota(jnp.int32, (tile, tile), 1) > lax.broadcasted_iota(
        jnp.int32, (tile, tile), 0
    )
    masks = jnp.concatenate([lower] * sharing, axis=0)

    def place_of(unit):
        turn, part = unit // tiles, unit % tiles
        head = turn % 2 * (heads // 2) + turn // 2
        start = pl.multiple_of(part * tile, tile)
        column = pl.multiple_of(head * head_width, HEAD_SIZE)
        return head, start, column

    def attend(unit):
        head, start, column = place_of(unit)
        taken = [
            pl.ds(pl.multiple_of(column + i * HEAD_SIZE, HEAD_SIZE), HEAD_SIZE)
            for i in range(sharing)
        ]
        stacked = jnp.concatenate([queries[pl.ds(start, tile), c] for c in taken], axis=0)
        key_columns = head_columns(head)

        def scores(index):
            keys = key_window[pl.ds(start + index * tile, tile), key_columns]
            return lax.dot_general(
                stacked, keys, (((1,), (1,)), ((), ())), preferred_element_type=jnp.float32
            )

        def mixed(index, weights):
            values = value_window[head, pl.ds(start + index * tile, tile), :]
            return jnp.dot(
                weights.astype(jnp.bfloat16), values, preferred_element_type=jnp.float32
            )

        edge = jnp.exp2(jnp.where(masks, scores(0), scores(reach)))
        total = mixed(0, jnp.where(masks, edge, 0.0))
        total = total + mixed(reach, jnp.where(masks, 0.0, edge))
        for index in range(1, reach):
            total = total + mixed(index, jnp.exp2(scores(index)))
        final = (total[:, :HEAD_SIZE] / total[:, HEAD_SIZE:]).astype(jnp.bfloat16)
        for i in range(sharing):
            attended[group, pl.ds(start, tile), taken[i]] = final[i * tile : (i + 1) * tile]

    def mixed_copy(unit, side):
        _, start, column = place_of(unit)
        piece = attended.at[side, pl.ds(start, tile), pl.ds(column, head_width)]
        return pltpu.make_async_remote_copy(
            src_ref=piece,
            dst_ref=piece,
            send_sem=mixed_send.at[unit],
            recv_sem=mixed_recv.at[unit],
            device_id=(me, 1 - group),
            device_id_type=MESH,
        )

    units = heads * tiles

    def attend_step(unit):
        attend(unit)

        @pl.when(unit > 0)
        def _():
            mixed_copy(unit - 1, group).start()

    def back_copy(chip, side):
        away = pl.multiple_of((1 - group) * part_rows, 16)
        return pltpu.make_async_remote_copy(
            src_ref=projected.at[chip, pl.ds(away, part_rows)],
            dst_ref=gathered.at[side, chip],
            send_sem=back_send.at[chip],
            recv_sem=back_recv.at[chip],
            device_id=(me, 1 - group),
            device_id_type=MESH,
        )

    def home_copy(chip):
        home = pl.multiple_of(group * part_rows, 16)
        return pltpu.make_async_copy(
            projected.at[chip, pl.ds(home, part_rows)], gathered.at[group, chip], home_sem.at[chip]
        )

    def project(way, step):
        chip = ring.owner(way, step)
        parts = [
            lax.dot_general(
                attended[side],
                pair_land[chip * 2 + side],
                (((1,), (1,)), ((), ())),
                preferred_element_type=jnp.float32,
            )
            for side in range(2)
        ]
        projected[chip] = (parts[0] + parts[1]).astype(jnp.bfloat16)
        home_copy(chip).start()
        back_copy(chip, group).start()

    steps(0, units // 2, attend_step)
    ring.hop(chips - 1, late, leave=[])
    query(late, chips - 2)
    query(late, chips - 1)
    finish_query(wide)
    finish_query(half + wide)
    steps(units // 2, units, attend_step)
    ring.hop(1, third)
    mixed_copy(units - 1, group).start()
    steps(0, units, lambda unit: mixed_copy(unit, 1 - group).wait_recv())
    ring.landed(origin, 0)
    project(1, 0)

    def both(step):
        ring.landed(third, step)
        project(1, step)
        project(-1, step)

    def third_step(step):
        both(step - 1)
        ring.hop(step, third)

    steps(2, middle - 1, third_step)
    both(middle - 2)
    ring.hop(middle - 1, third, leave=farthest)
    both(middle - 1)
    ring.hop(middle, farthest, leave=[])
    ring.landed(farthest, middle)
    project(1, middle)
    steps(0, chips, lambda chip: back_copy(chip, 1 - group).wait_recv())

    for index, part in stacks:

        @pl.when(me + 2 < shards)
        def _():
            far_copy(index, part).wait_send()

        @pl.when(core == 0)
        def _():
            near_copy(index, part, blocks - 1).wait_send()

        @pl.when(core == 1)
        def _():
            @pl.when(me >= 2)
            def _():
                near_copy(index, part, 0).wait_send()

    for piece in range(token_pieces):
        token_copy(piece, group).wait_send()
    steps(0, chips - 1, lambda step: ring.sent(step, second, second))
    ring.sent(chips - 1, [], second)
    ring.sent(0, third, origin)
    steps(1, middle - 1, lambda step: ring.sent(step, third, third))
    ring.sent(middle - 1, farthest, third)
    ring.sent(middle, [], farthest)
    steps(0, units, lambda unit: mixed_copy(unit, group).wait_send())
    steps(0, chips, lambda chip: back_copy(chip, group).wait_send())
    steps(0, chips, lambda chip: home_copy(chip).wait())


def final_kernel(gathered_ref, tokens_ref, gain_ref, result_ref):
    sides, chips, rows, _ = gathered_ref.shape
    block = 32
    gain = gain_ref[...][None, :]

    def one(index):
        span = pl.ds(pl.multiple_of(index * block, block), block)
        values = jnp.concatenate(
            [
                gathered_ref[side, chip, span, :].astype(jnp.float32)
                for chip in range(chips)
                for side in range(sides)
            ],
            axis=1,
        )
        mean_square = jnp.mean(values * values, axis=-1, keepdims=True)
        scaled = values * lax.rsqrt(mean_square + epsilon) * gain
        result_ref[span, :] = (tokens_ref[span, :].astype(jnp.float32) + scaled).astype(
            jnp.bfloat16
        )

    steps(0, rows // block, one)


def on_device(
    tokens,
    norm_gain,
    query_weight,
    key_matrix,
    value_matrix,
    out_weight,
    query_gain,
    key_gain,
    post_gain,
):
    shards = lax.axis_size("seq")
    copies = lax.axis_size("fsdp")
    chips = shards // 2
    part_rows, model_width = tokens.shape
    shard_rows = part_rows * copies
    rows, query_width = query_weight.shape
    key_width = key_matrix.shape[1]
    merge = 2 if rows % 16 == 0 else 1
    heads = key_width // HEAD_SIZE
    units = heads * copies
    window = WINDOW_LENGTH + shard_rows

    hbm = pl.BlockSpec(memory_space=pltpu.MemorySpace.HBM)
    vmem = pl.BlockSpec(memory_space=pltpu.VMEM)
    bf16, f32 = jnp.bfloat16, jnp.float32
    dma = pltpu.SemaphoreType.DMA
    gathered, _ = pl.pallas_call(
        functools.partial(layer_kernel, shards, merge),
        out_shape=[
            jax.ShapeDtypeStruct((copies, chips, part_rows, rows), bf16),
            jax.ShapeDtypeStruct(out_weight.shape, bf16),
        ],
        in_specs=[hbm, vmem, hbm, hbm, hbm, hbm, vmem, vmem],
        out_specs=[hbm, hbm],
        scratch_shapes=[
            pltpu.VMEM((shards, rows, query_width), bf16),
            pltpu.VMEM((shards, rows, query_width), bf16),
            pltpu.VMEM((copies, part_rows, model_width), bf16),
            pltpu.VMEM((shards // merge, shard_rows, merge * rows), bf16),
            pltpu.VMEM((shard_rows, query_width), f32),
            pltpu.VMEM((shard_rows, key_width), f32),
            pltpu.VMEM((shard_rows, key_width), f32),
            pltpu.VMEM((shard_rows, query_width), bf16),
            pltpu.VMEM((window, key_width), bf16),
            pltpu.VMEM((heads, window, 2 * HEAD_SIZE), bf16),
            pltpu.VMEM((copies, shard_rows, query_width), bf16),
            pltpu.VMEM((chips, shard_rows, rows), bf16),
            pltpu.VMEM((shard_rows, HEAD_SIZE), f32),
            pltpu.VMEM((shard_rows, HEAD_SIZE), f32),
            *[dma((4 * pieces + 4, chips))] * 4,
            dma((4,)),
            dma((token_pieces,)),
            dma((token_pieces,)),
            dma((2,)),
            dma((2,)),
            dma((2,)),
            dma((2,)),
            dma((2,)),
            dma((units,)),
            dma((units,)),
            dma((chips,)),
            dma((chips,)),
            dma((chips,)),
            pltpu.SemaphoreType.REGULAR,
        ],
        compiler_params=pltpu.CompilerParams(
            collective_id=0, has_side_effects=True, vmem_limit_bytes=67043328
        ),
    )(
        tokens,
        norm_gain,
        query_weight,
        key_matrix,
        value_matrix,
        out_weight,
        query_gain,
        key_gain,
    )
    tile = 64
    return pl.pallas_call(
        final_kernel,
        out_shape=jax.ShapeDtypeStruct(tokens.shape, bf16),
        grid=(part_rows // tile,),
        in_specs=[
            pl.BlockSpec((copies, chips, tile, rows), lambda i: (0, 0, i, 0)),
            pl.BlockSpec((tile, model_width), lambda i: (i, 0)),
            pl.BlockSpec((model_width,), lambda i: (0,)),
        ],
        out_specs=pl.BlockSpec((tile, model_width), lambda i: (i, 0)),
    )(gathered, tokens, post_gain)


def solution(mesh):
    in_specs = (
        P(("seq", "fsdp"), None),
        P(),
        P("seq", "fsdp"),
        P("seq", "fsdp"),
        P("seq", "fsdp"),
        P("seq", "fsdp"),
        P(),
        P(),
        P(),
    )
    out_specs = P(("seq", "fsdp"), None)
    return jax.shard_map(
        on_device, mesh=mesh, in_specs=in_specs, out_specs=out_specs, check_vma=False
    )
```

```python
import functools
import math

import jax
import jax.numpy as jnp
from jax import lax
from jax.experimental import pallas as pl
from jax.experimental.pallas import tpu as pltpu
from jax.sharding import PartitionSpec as P

HEAD_SIZE = 128
WINDOW_LENGTH = 1024

epsilon = 1e-06
score_scale = 168.0 ** (-0.5)
log2_e = 1.4426950408889634
rope_base = 10000.0
pieces = 2
token_pieces = 4
MESH = pl.DeviceIdType.MESH


def ring_place(chip, chips):
    row, side = chip // 2, chip % 2
    return side * (chips - 1 - row) + (1 - side) * row


def ring_chip(place, chips):
    back = place // (chips // 2)
    return back * (2 * (chips - 1 - place) + 1) + (1 - back) * 2 * place


class Ring:
    def __init__(self, shards, sems):
        self.chips = shards // 2
        self.me = lax.axis_index("seq")
        self.group = lax.axis_index("fsdp")
        self.core = self.me % 2
        self.place = ring_place(self.me // 2, self.chips)
        self.other = (self.me // 2) * 2 + 1 - self.core
        self.ahead = self.neighbour(1)
        self.behind = self.neighbour(self.chips - 1)
        self.ring_send, self.ring_recv, self.pair_send, self.pair_recv = sems

    def neighbour(self, distance):
        return ring_chip((self.place + distance) % self.chips, self.chips) * 2 + self.core

    def owner(self, way, step):
        return ring_chip((self.place + (self.chips - way) * step) % self.chips, self.chips)

    def ring_copy(self, flow, step, sent):
        index, slot_of, way = flow
        slot = slot_of(self.owner(way, step), self.core)
        return pltpu.make_async_remote_copy(
            src_ref=slot,
            dst_ref=slot,
            send_sem=self.ring_send.at[index, sent],
            recv_sem=self.ring_recv.at[index, sent],
            device_id=(self.ahead if way > 0 else self.behind, self.group),
            device_id_type=MESH,
        )

    def pair_copy(self, flow, step, core):
        index, slot_of, way = flow
        slot = slot_of(self.owner(way, step), core)
        return pltpu.make_async_remote_copy(
            src_ref=slot,
            dst_ref=slot,
            send_sem=self.pair_send.at[index, step],
            recv_sem=self.pair_recv.at[index, step],
            device_id=(self.other, self.group),
            device_id_type=MESH,
        )

    def hop(self, step, flows, arrive=None, leave=None, hand=None):
        for flow in flows:
            if arrive is None or flow in arrive:
                self.ring_copy(flow, step, step - 1).wait_recv()
            if leave is None or flow in leave:
                self.ring_copy(flow, step, step).start()
            if hand is None or flow in hand:
                self.pair_copy(flow, step, self.core).start()

    def landed(self, flows, step):
        for flow in flows:
            self.pair_copy(flow, step, 1 - self.core).wait_recv()

    def sent(self, step, leave, hand):
        for flow in leave:
            self.ring_copy(flow, step, step).wait_send()
        for flow in hand:
            self.pair_copy(flow, step, self.core).wait_send()


def steps(first, last, body):
    def one(step, carry):
        body(step)
        return carry

    lax.fori_loop(first, last, one, 0)


def turned(values, gain, cosine, sine, scale):
    mean_square = jnp.mean(values * values, axis=-1, keepdims=True)
    normed = values * lax.rsqrt(mean_square + epsilon) * gain
    swapped = pltpu.roll(normed, values.shape[-1] // 2, 1)
    return (normed * cosine + swapped * sine) * scale


def layer_kernel(
    shards,
    merge,
    tokens_ref,
    gain_ref,
    query_ref,
    key_ref,
    value_ref,
    out_ref,
    query_gain_ref,
    key_gain_ref,
    gathered,
    swap_out,
    query_land,
    pair_land,
    raw,
    split,
    query_sum,
    key_sum,
    value_sum,
    queries,
    key_window,
    value_window,
    attended,
    projected,
    cosines,
    sines,
    ring_send,
    ring_recv,
    pair_send,
    pair_recv,
    local_sem,
    token_send,
    token_recv,
    swap_sem,
    far_send,
    far_recv,
    near_send,
    near_recv,
    mixed_send,
    mixed_recv,
    back_send,
    back_recv,
    home_sem,
    free_sem,
):
    ring = Ring(shards, (ring_send, ring_recv, pair_send, pair_recv))
    chips, me, group, core = ring.chips, ring.me, ring.group, ring.core
    rows, width = key_ref.shape
    part_rows = tokens_ref.shape[0]
    columns = query_ref.shape[1]
    half = columns // 2
    shard_rows = queries.shape[0]
    heads = width // HEAD_SIZE
    query_heads = columns // HEAD_SIZE
    sharing = query_heads // heads
    head_width = sharing * HEAD_SIZE
    blocks = WINDOW_LENGTH // shard_rows + 1
    far_to = (me + 2) % shards
    far_from = (me + shards - 2) % shards
    middle = chips // 2

    barrier = pltpu.get_barrier_semaphore()
    for device in (ring.other, ring.ahead, ring.behind, far_to, far_from):
        pl.semaphore_signal(barrier, inc=1, device_id=(device, group), device_id_type=MESH)
    pl.semaphore_signal(barrier, inc=1, device_id=(me, 1 - group), device_id_type=MESH)

    @pl.when(core != group)
    def _():
        pl.semaphore_signal(
            barrier,
            inc=1,
            device_id=((me // 2) * 2 + group, core),
            device_id_type=MESH,
        )

    local = [
        pltpu.make_async_copy(key_ref, pair_land.at[me, :, pl.ds(0, width)], local_sem.at[0]),
        pltpu.make_async_copy(
            value_ref, pair_land.at[me, :, pl.ds(width, width)], local_sem.at[1]
        ),
        pltpu.make_async_copy(query_ref, query_land.at[me], local_sem.at[2]),
        pltpu.make_async_copy(tokens_ref, raw.at[group], local_sem.at[3]),
    ]
    for copy in local:
        copy.start()
    pl.semaphore_wait(barrier, 6 + (core + group) % 2)

    def flow(index, land, column, count, way):
        return index, lambda chip, side: land.at[chip * 2 + side, :, pl.ds(column, count)], way

    size, wide = width // pieces, half // pieces
    first, second = [], []
    for piece in range(pieces):
        first.append(flow(2 * piece, pair_land, piece * size, size, 1))
        first.append(flow(2 * piece + 1, pair_land, width + piece * size, size, -1))
    for piece in range(pieces):
        base = 2 * (pieces + piece)
        second.append(flow(base, query_land, piece * wide, wide, 1))
        second.append(flow(base + 1, query_land, half + piece * wide, wide, -1))
    third = []
    for piece in range(2):
        for way in (1, -1):
            third.append(flow(4 * pieces + len(third), pair_land, piece * half, half, way))
    origin = [third[0], third[2]]
    farthest = [third[0], third[3]]

    token_rows = part_rows // token_pieces

    def token_copy(piece, side):
        span = pl.ds(piece * token_rows, token_rows)
        return pltpu.make_async_remote_copy(
            src_ref=tokens_ref.at[span],
            dst_ref=raw.at[side, span],
            send_sem=token_send.at[piece],
            recv_sem=token_recv.at[piece],
            device_id=(me, 1 - group),
            device_id_type=MESH,
        )

    swap = pltpu.make_async_remote_copy(
        src_ref=out_ref,
        dst_ref=swap_out,
        send_sem=swap_sem.at[0],
        recv_sem=swap_sem.at[1],
        device_id=((me // 2) * 2 + group, core),
        device_id_type=MESH,
    )

    local[0].wait()
    local[1].wait()
    ring.hop(0, first, arrive=[])
    for piece in range(token_pieces):
        token_copy(piece, group).start()

    @pl.when(core != group)
    def _():
        swap.start()

    local[2].wait()
    local[3].wait()

    block = 16
    span_width = rows * merge

    def normed_rows(side, begin, count):
        def one(index):
            start = pl.multiple_of(begin + index * block, block)
            values = raw[side, pl.ds(start, block), :].astype(jnp.float32)
            mean_square = jnp.mean(values * values, axis=-1, keepdims=True)
            normed = values * lax.rsqrt(mean_square + epsilon) * gain_ref[...][None, :]
            target = pl.multiple_of(side * part_rows + start, block)
            for part in range(shards // merge):
                piece = normed[:, part * span_width : (part + 1) * span_width]
                split[part, pl.ds(target, block), :] = piece.astype(jnp.bfloat16)

        steps(0, count // block, one)

    normed_rows(group, 0, part_rows)
    key_sum[...] = jnp.zeros_like(key_sum)
    value_sum[...] = jnp.zeros_like(value_sum)
    query_sum[...] = jnp.zeros_like(query_sum)
    lanes = lax.broadcasted_iota(jnp.int32, (shard_rows, HEAD_SIZE), 1)
    positions = me * shard_rows + lax.broadcasted_iota(jnp.int32, (shard_rows, HEAD_SIZE), 0)
    exponents = (lanes % (HEAD_SIZE // 2)).astype(jnp.float32) * (2.0 / HEAD_SIZE)
    angles = positions.astype(jnp.float32) * jnp.exp(-exponents * math.log(rope_base))
    cosines[...] = jnp.cos(angles)
    turn = jnp.sin(angles)
    sines[...] = jnp.where(lanes < HEAD_SIZE // 2, -turn, turn)

    for slot in range(blocks - 1):
        distance = blocks - 1 - slot
        span = pl.ds(slot * shard_rows, shard_rows)

        @pl.when(me < distance)
        def _():
            key_window[span, :] = jnp.zeros((shard_rows, width), jnp.bfloat16)
            for head in range(heads):
                value_window[head, span, :] = jnp.zeros(
                    (shard_rows, 2 * HEAD_SIZE), jnp.bfloat16
                )

    for slot in range(blocks):
        span = pl.ds(slot * shard_rows, shard_rows)

        @pl.when(me >= blocks - 1 - slot)
        def _():
            for head in range(heads):
                value_window[head, span, pl.ds(HEAD_SIZE, HEAD_SIZE)] = jnp.ones(
                    (shard_rows, HEAD_SIZE), jnp.bfloat16
                )

    def products(total, begin, land, column, count, chip):
        target = pl.ds(begin, count)
        taken = pl.ds(column, count)
        if merge == 2:
            weights = land[pl.ds(chip * 2, 2), :, taken].reshape(2 * rows, count)
            total[:, target] += jnp.dot(
                split[chip], weights, preferred_element_type=jnp.float32
            )
        else:
            for side in range(2):
                total[:, target] += jnp.dot(
                    split[chip * 2 + side],
                    land[chip * 2 + side, :, taken],
                    preferred_element_type=jnp.float32,
                )

    def key_value(step):
        products(key_sum, 0, pair_land, 0, width, ring.owner(1, step))
        products(value_sum, 0, pair_land, width, width, ring.owner(-1, step))

    def query(flows, step):
        column = flows[0][0] // 2 % pieces * wide
        ring.landed(flows, step)
        products(query_sum, column, query_land, column, wide, ring.owner(1, step))
        column += half
        products(query_sum, column, query_land, column, wide, ring.owner(-1, step))

    early, late = second[:2], second[2:]

    steps(1, chips - 4, lambda step: ring.hop(step, first))
    ring.hop(chips - 4, first)
    ring.hop(0, early, arrive=[])
    ring.hop(chips - 3, first)
    ring.hop(1, early)
    ring.hop(chips - 2, first)
    ring.hop(2, early)
    ring.hop(0, late, arrive=[])
    ring.hop(chips - 1, first, leave=[])
    ring.hop(3, early)
    for piece in range(token_pieces - 1):
        token_copy(piece, 1 - group).wait_recv()
    normed_rows(1 - group, 0, part_rows - token_rows)
    steps(0, chips, lambda step: ring.landed(first, step))

    def span_of(slot):
        return pl.ds(slot * shard_rows, shard_rows)

    def key_part(slot):
        return key_window.at[span_of(slot)]

    def value_part(slot):
        return value_window.at[:, span_of(slot), pl.ds(0, HEAD_SIZE)]

    stacks = ((0, key_part), (1, value_part))

    def far_copy(index, part):
        return pltpu.make_async_remote_copy(
            src_ref=part(blocks - 1),
            dst_ref=part(0),
            send_sem=far_send.at[index],
            recv_sem=far_recv.at[index],
            device_id=(far_to, group),
            device_id_type=MESH,
        )

    def near_copy(index, part, slot):
        return pltpu.make_async_remote_copy(
            src_ref=part(slot),
            dst_ref=part(1),
            send_sem=near_send.at[index],
            recv_sem=near_recv.at[index],
            device_id=(ring.other, group),
            device_id_type=MESH,
        )

    def head_columns(head):
        return pl.ds(pl.multiple_of(head * HEAD_SIZE, HEAD_SIZE), HEAD_SIZE)

    def finish_keys():
        def one(head):
            taken = head_columns(head)
            key_window[span_of(blocks - 1), taken] = turned(
                key_sum[:, taken], key_gain_ref[...][None, :], cosines[...], sines[...], 1.0
            ).astype(jnp.bfloat16)
            value_window[head, span_of(blocks - 1), pl.ds(0, HEAD_SIZE)] = value_sum[
                :, taken
            ].astype(jnp.bfloat16)

        steps(0, heads, one)

    def send_keys():
        for index, part in stacks:

            @pl.when(me + 2 < shards)
            def _():
                far_copy(index, part).start()

            @pl.when(core == 0)
            def _():
                near_copy(index, part, blocks - 1).start()

    def own_copy(source):
        return pltpu.make_async_copy(source, pair_land.at[me], local_sem.at[0])

    def free_slots():
        steps(0, chips - 1, lambda step: ring.sent(step, first, first))
        ring.sent(chips - 1, [], first)
        for device in (ring.other, ring.ahead, ring.behind):
            pl.semaphore_signal(
                free_sem, inc=1, device_id=(device, group), device_id_type=MESH
            )

        @pl.when(core == group)
        def _():
            own_copy(out_ref).start()

        @pl.when(core != group)
        def _():
            swap.wait()
            own_copy(swap_out).start()

    def second_step(step):
        ring.hop(step + 3, early)
        ring.hop(step, late)

        @pl.when(step == 1)
        def _():
            token_copy(token_pieces - 1, 1 - group).wait_recv()
            normed_rows(1 - group, part_rows - token_rows, token_rows)
            steps(0, middle, key_value)

        @pl.when(step == 2)
        def _():
            steps(middle, chips, key_value)
            finish_keys()

        @pl.when(step == 3)
        def _():
            query(early, 0)
            send_keys()
            steps(1, 5, lambda step: query(early, step))
            steps(0, 3, lambda step: query(late, step))

        @pl.when(step > 3)
        def _():
            query(early, step + 1)
            query(late, step - 1)

    def finish_query(column):
        def one(head):
            taken = pl.ds(pl.multiple_of(column + head * HEAD_SIZE, HEAD_SIZE), HEAD_SIZE)
            queries[:, taken] = turned(
                query_sum[:, taken],
                query_gain_ref[...][None, :],
                cosines[...],
                sines[...],
                score_scale * log2_e,
            ).astype(jnp.bfloat16)

        steps(0, wide // HEAD_SIZE, one)

    steps(1, chips - 4, second_step)
    ring.hop(chips - 1, early, leave=[])
    ring.hop(chips - 4, late)
    query(early, chips - 3)
    query(early, chips - 2)
    query(early, chips - 1)
    finish_query(0)
    finish_query(half)
    query(late, chips - 5)
    free_slots()
    ring.hop(chips - 3, late)
    query(late, chips - 4)
    ring.hop(chips - 2, late)
    pl.semaphore_wait(free_sem, 3)
    own_copy(out_ref).wait()
    ring.hop(0, third, arrive=[], hand=origin)
    query(late, chips - 3)

    @pl.when(me >= 2)
    def _():
        for index, part in stacks:
            far_copy(index, part).wait_recv()

            @pl.when(core == 1)
            def _():
                near_copy(index, part, 0).start()

    for index, part in stacks:

        @pl.when(core == 1)
        def _():
            near_copy(index, part, 0).wait_recv()

        @pl.when(core == 0)
        def _():
            @pl.when(me >= 2)
            def _():
                near_copy(index, part, 0).wait_recv()

    tile = part_rows
    tiles = shard_rows // tile
    reach = WINDOW_LENGTH // tile
    lower = lax.broadcasted_iota(jnp.int32, (tile, tile), 1) > lax.broadcasted_iota(
        jnp.int32, (tile, tile), 0
    )
    masks = jnp.concatenate([lower] * sharing, axis=0)

    def place_of(unit):
        turn, part = unit // tiles, unit % tiles
        head = turn % 2 * (heads // 2) + turn // 2
        start = pl.multiple_of(part * tile, tile)
        column = pl.multiple_of(head * head_width, HEAD_SIZE)
        return head, start, column

    def attend(unit):
        head, start, column = place_of(unit)
        taken = [
            pl.ds(pl.multiple_of(column + i * HEAD_SIZE, HEAD_SIZE), HEAD_SIZE)
            for i in range(sharing)
        ]
        stacked = jnp.concatenate([queries[pl.ds(start, tile), c] for c in taken], axis=0)
        key_columns = head_columns(head)

        def scores(index):
            keys = key_window[pl.ds(start + index * tile, tile), key_columns]
            return lax.dot_general(
                stacked, keys, (((1,), (1,)), ((), ())), preferred_element_type=jnp.float32
            )

        def mixed(index, weights):
            values = value_window[head, pl.ds(start + index * tile, tile), :]
            return jnp.dot(
                weights.astype(jnp.bfloat16), values, preferred_element_type=jnp.float32
            )

        edge = jnp.exp2(jnp.where(masks, scores(0), scores(reach)))
        total = mixed(0, jnp.where(masks, edge, 0.0))
        total = total + mixed(reach, jnp.where(masks, 0.0, edge))
        for index in range(1, reach):
            total = total + mixed(index, jnp.exp2(scores(index)))
        final = (total[:, :HEAD_SIZE] / total[:, HEAD_SIZE:]).astype(jnp.bfloat16)
        for i in range(sharing):
            attended[group, pl.ds(start, tile), taken[i]] = final[i * tile : (i + 1) * tile]

    def mixed_copy(unit, side):
        _, start, column = place_of(unit)
        piece = attended.at[side, pl.ds(start, tile), pl.ds(column, head_width)]
        return pltpu.make_async_remote_copy(
            src_ref=piece,
            dst_ref=piece,
            send_sem=mixed_send.at[unit],
            recv_sem=mixed_recv.at[unit],
            device_id=(me, 1 - group),
            device_id_type=MESH,
        )

    units = heads * tiles

    def attend_step(unit):
        attend(unit)

        @pl.when(unit > 0)
        def _():
            mixed_copy(unit - 1, group).start()

    def back_copy(chip, side):
        away = pl.multiple_of((1 - group) * part_rows, 16)
        return pltpu.make_async_remote_copy(
            src_ref=projected.at[chip, pl.ds(away, part_rows)],
            dst_ref=gathered.at[side, chip],
            send_sem=back_send.at[chip],
            recv_sem=back_recv.at[chip],
            device_id=(me, 1 - group),
            device_id_type=MESH,
        )

    def home_copy(chip):
        home = pl.multiple_of(group * part_rows, 16)
        return pltpu.make_async_copy(
            projected.at[chip, pl.ds(home, part_rows)], gathered.at[group, chip], home_sem.at[chip]
        )

    def project_rows(chip, side_of_pair):
        span = pl.ds(pl.multiple_of(side_of_pair * part_rows, 16), part_rows)
        parts = [
            lax.dot_general(
                attended[side, span, :],
                pair_land[chip * 2 + side],
                (((1,), (1,)), ((), ())),
                preferred_element_type=jnp.float32,
            )
            for side in range(2)
        ]
        projected[chip, span, :] = (parts[0] + parts[1]).astype(jnp.bfloat16)

    def project(way, step):
        chip = ring.owner(way, step)
        parts = [
            lax.dot_general(
                attended[side],
                pair_land[chip * 2 + side],
                (((1,), (1,)), ((), ())),
                preferred_element_type=jnp.float32,
            )
            for side in range(2)
        ]
        projected[chip] = (parts[0] + parts[1]).astype(jnp.bfloat16)
        home_copy(chip).start()
        back_copy(chip, group).start()

    steps(0, units // 2, attend_step)
    ring.hop(chips - 1, late, leave=[])
    query(late, chips - 2)
    query(late, chips - 1)
    finish_query(wide)
    finish_query(half + wide)
    ring.hop(1, third[:2])
    steps(units // 2, units, attend_step)
    ring.hop(1, third[2:])
    mixed_copy(units - 1, group).start()
    steps(0, units, lambda unit: mixed_copy(unit, 1 - group).wait_recv())
    ring.landed(origin, 0)
    project(1, 0)

    def both(step):
        ring.landed(third, step)
        project(1, step)
        project(-1, step)

    def third_step(step):
        both(step - 1)
        ring.hop(step, third)

    steps(2, middle - 1, third_step)
    both(middle - 2)
    ring.hop(middle - 1, third, leave=farthest)
    both(middle - 1)
    ring.hop(middle, farthest, leave=[])
    ring.landed(farthest, middle)
    last = ring.owner(1, middle)
    project_rows(last, 1 - group)
    back_copy(last, group).start()
    project_rows(last, group)
    home_copy(last).start()
    steps(0, chips, lambda chip: back_copy(chip, 1 - group).wait_recv())

    for index, part in stacks:

        @pl.when(me + 2 < shards)
        def _():
            far_copy(index, part).wait_send()

        @pl.when(core == 0)
        def _():
            near_copy(index, part, blocks - 1).wait_send()

        @pl.when(core == 1)
        def _():
            @pl.when(me >= 2)
            def _():
                near_copy(index, part, 0).wait_send()

    for piece in range(token_pieces):
        token_copy(piece, group).wait_send()
    steps(0, chips - 1, lambda step: ring.sent(step, second, second))
    ring.sent(chips - 1, [], second)
    ring.sent(0, third, origin)
    steps(1, middle - 1, lambda step: ring.sent(step, third, third))
    ring.sent(middle - 1, farthest, third)
    ring.sent(middle, [], farthest)
    steps(0, units, lambda unit: mixed_copy(unit, group).wait_send())
    steps(0, chips, lambda chip: back_copy(chip, group).wait_send())
    steps(0, chips, lambda chip: home_copy(chip).wait())


def final_kernel(gathered_ref, tokens_ref, gain_ref, result_ref):
    sides, chips, rows, _ = gathered_ref.shape
    block = 32
    gain = gain_ref[...][None, :]

    def one(index):
        span = pl.ds(pl.multiple_of(index * block, block), block)
        values = jnp.concatenate(
            [
                gathered_ref[side, chip, span, :].astype(jnp.float32)
                for chip in range(chips)
                for side in range(sides)
            ],
            axis=1,
        )
        mean_square = jnp.mean(values * values, axis=-1, keepdims=True)
        scaled = values * lax.rsqrt(mean_square + epsilon) * gain
        result_ref[span, :] = (tokens_ref[span, :].astype(jnp.float32) + scaled).astype(
            jnp.bfloat16
        )

    steps(0, rows // block, one)


def on_device(
    tokens,
    norm_gain,
    query_weight,
    key_matrix,
    value_matrix,
    out_weight,
    query_gain,
    key_gain,
    post_gain,
):
    shards = lax.axis_size("seq")
    copies = lax.axis_size("fsdp")
    chips = shards // 2
    part_rows, model_width = tokens.shape
    shard_rows = part_rows * copies
    rows, query_width = query_weight.shape
    key_width = key_matrix.shape[1]
    merge = 2 if rows % 16 == 0 else 1
    heads = key_width // HEAD_SIZE
    units = heads * copies
    window = WINDOW_LENGTH + shard_rows

    hbm = pl.BlockSpec(memory_space=pltpu.MemorySpace.HBM)
    vmem = pl.BlockSpec(memory_space=pltpu.VMEM)
    bf16, f32 = jnp.bfloat16, jnp.float32
    dma = pltpu.SemaphoreType.DMA
    gathered, _ = pl.pallas_call(
        functools.partial(layer_kernel, shards, merge),
        out_shape=[
            jax.ShapeDtypeStruct((copies, chips, part_rows, rows), bf16),
            jax.ShapeDtypeStruct(out_weight.shape, bf16),
        ],
        in_specs=[hbm, vmem, hbm, hbm, hbm, hbm, vmem, vmem],
        out_specs=[hbm, hbm],
        scratch_shapes=[
            pltpu.VMEM((shards, rows, query_width), bf16),
            pltpu.VMEM((shards, rows, query_width), bf16),
            pltpu.VMEM((copies, part_rows, model_width), bf16),
            pltpu.VMEM((shards // merge, shard_rows, merge * rows), bf16),
            pltpu.VMEM((shard_rows, query_width), f32),
            pltpu.VMEM((shard_rows, key_width), f32),
            pltpu.VMEM((shard_rows, key_width), f32),
            pltpu.VMEM((shard_rows, query_width), bf16),
            pltpu.VMEM((window, key_width), bf16),
            pltpu.VMEM((heads, window, 2 * HEAD_SIZE), bf16),
            pltpu.VMEM((copies, shard_rows, query_width), bf16),
            pltpu.VMEM((chips, shard_rows, rows), bf16),
            pltpu.VMEM((shard_rows, HEAD_SIZE), f32),
            pltpu.VMEM((shard_rows, HEAD_SIZE), f32),
            *[dma((4 * pieces + 4, chips))] * 4,
            dma((4,)),
            dma((token_pieces,)),
            dma((token_pieces,)),
            dma((2,)),
            dma((2,)),
            dma((2,)),
            dma((2,)),
            dma((2,)),
            dma((units,)),
            dma((units,)),
            dma((chips,)),
            dma((chips,)),
            dma((chips,)),
            pltpu.SemaphoreType.REGULAR,
        ],
        compiler_params=pltpu.CompilerParams(
            collective_id=0, has_side_effects=True, vmem_limit_bytes=67043328
        ),
    )(
        tokens,
        norm_gain,
        query_weight,
        key_matrix,
        value_matrix,
        out_weight,
        query_gain,
        key_gain,
    )
    tile = 64
    return pl.pallas_call(
        final_kernel,
        out_shape=jax.ShapeDtypeStruct(tokens.shape, bf16),
        grid=(part_rows // tile,),
        in_specs=[
            pl.BlockSpec((copies, chips, tile, rows), lambda i: (0, 0, i, 0)),
            pl.BlockSpec((tile, model_width), lambda i: (i, 0)),
            pl.BlockSpec((model_width,), lambda i: (0,)),
        ],
        out_specs=pl.BlockSpec((tile, model_width), lambda i: (i, 0)),
    )(gathered, tokens, post_gain)


def solution(mesh):
    in_specs = (
        P(("seq", "fsdp"), None),
        P(),
        P("seq", "fsdp"),
        P("seq", "fsdp"),
        P("seq", "fsdp"),
        P("seq", "fsdp"),
        P(),
        P(),
        P(),
    )
    out_specs = P(("seq", "fsdp"), None)
    return jax.shard_map(
        on_device, mesh=mesh, in_specs=in_specs, out_specs=out_specs, check_vma=False
    )
```
